32 devices in a mesh: pairs: 1 (over z), ho: 4 (over y), tp: 8 (over x, core).
Axes of the slice: x: 4, y: 4, z: 1, core: 2. Of those that a mesh axis runs over, the one named last changes fastest.
The devices are a block of a 4x4x8 slice.
Arguments:
- prompts: bfloat16 [4, 2048, 4096], P('pairs')
- y_first: bfloat16 [4, 4096], P(('pairs', 'ho'))
- w_qkv: bfloat16 [2, 4096, 8, 6, 128], P(None, None, 'tp')
- w_o: bfloat16 [2, 4096, 4096], P(None, 'tp')
- w_gate: bfloat16 [2, 4096, 12288], P(None, None, 'tp')
- w_up: bfloat16 [2, 4096, 12288], P(None, None, 'tp')
- w_down: bfloat16 [2, 12288, 4096], P(None, 'tp')
- g_attn: float32 [2, 4096], replicated
- g_mlp: float32 [2, 4096], replicated
Outputs:
- output 1: bfloat16 [4, 2048, 4096], P(('pairs', 'ho'))
- output 2: float32 [4, 4096], P(('pairs', 'ho'))
- output 3: bfloat16 [4, 2, 2048, 8, 128], P(('pairs', 'ho'), None, 'tp')
- output 4: bfloat16 [4, 2, 2048, 8, 128], P(('pairs', 'ho'), None, 'tp')
- output 5: bfloat16 [4, 2, 2, 8, 128], P(('pairs', 'ho'), None, None, 'tp')
All inputs are finite; a program needn't handle non-finite values.
Results may differ from the reference program's by a relative error of at most 0.02.
Values are sent between devices in bfloat16 or wider.
A program may use at most 768 MiB of HBM per device.

```python
import math
import jax
import jax.numpy as jnp
from jax import lax

D = 4096
HEADS = 32
KV_HEADS = 8
HEAD = 128
FF = 12288
TOKENS = 2048
LAYERS = 2
INST = 4

GROUP = HEADS // KV_HEADS
NORM_EPS = 1e-5


def setup_inputs(seed: int = 0, part: int = 0) -> dict:
    w_keys = jax.random.split(jax.random.key(seed), 7)
    p_keys = jax.random.split(jax.random.fold_in(jax.random.key(seed + 1), part), 2)
    q_gain = math.sqrt(0.4 * math.log(TOKENS))
    slot_gain = jnp.concatenate([jnp.full((GROUP,), q_gain, jnp.float32), jnp.ones((2,), jnp.float32)])
    prompts = jax.random.normal(p_keys[0], (INST, TOKENS, D), jnp.float32)
    y_first = jax.random.normal(p_keys[1], (INST, D), jnp.float32)
    w_qkv = jax.random.normal(w_keys[0], (LAYERS, D, KV_HEADS, GROUP + 2, HEAD), jnp.float32) * (D ** -0.5) * slot_gain[:, None]
    w_o = jax.random.normal(w_keys[1], (LAYERS, HEADS * HEAD, D), jnp.float32) * (2.0 * (HEADS * HEAD) ** -0.5)
    w_gate = jax.random.normal(w_keys[2], (LAYERS, D, FF), jnp.float32) * (D ** -0.5)
    w_up = jax.random.normal(w_keys[3], (LAYERS, D, FF), jnp.float32) * (D ** -0.5)
    w_down = jax.random.normal(w_keys[4], (LAYERS, FF, D), jnp.float32) * (FF ** -0.5)
    g_attn = jax.random.uniform(w_keys[5], (LAYERS, D), jnp.float32, 0.5, 1.5)
    g_mlp = jax.random.uniform(w_keys[6], (LAYERS, D), jnp.float32, 0.5, 1.5)
    return {'prompts': prompts.astype(jnp.bfloat16), 'y_first': y_first.astype(jnp.bfloat16), 'w_qkv': w_qkv.astype(jnp.bfloat16), 'w_o': w_o.astype(jnp.bfloat16), 'w_gate': w_gate.astype(jnp.bfloat16), 'w_up': w_up.astype(jnp.bfloat16), 'w_down': w_down.astype(jnp.bfloat16), 'g_attn': g_attn, 'g_mlp': g_mlp}


def rms_norm(hidden, gain_vec):
    widened = hidden.astype(jnp.float32)
    inv_rms = lax.rsqrt(jnp.mean(widened * widened, axis=-1, keepdims=True) + NORM_EPS)
    return (widened * inv_rms * gain_vec).astype(jnp.bfloat16)


def mlp_block(h_mlp, w_gate, w_up, w_down):
    gate_pre = jnp.dot(h_mlp, w_gate, preferred_element_type=jnp.float32)
    up_pre = jnp.dot(h_mlp, w_up, preferred_element_type=jnp.float32)
    act_mid = (jax.nn.silu(gate_pre) * up_pre).astype(jnp.bfloat16)
    return jnp.dot(act_mid, w_down, preferred_element_type=jnp.float32).astype(jnp.bfloat16)


def causal_attention(queries, key_rows, val_rows):
    positions = jnp.arange(TOKENS)
    allowed = positions[:, None] >= positions[None, :]

    def one_group(operands):
        q_grp, k_one, v_one = operands
        scores = jnp.einsum('tgh,sh->gts', q_grp.astype(jnp.float32), k_one.astype(jnp.float32)) * (HEAD ** -0.5)
        scores = jnp.where(allowed[None], scores, -jnp.inf)
        weights = jnp.exp(scores - jnp.max(scores, axis=-1, keepdims=True))
        denom_sum = jnp.sum(weights, axis=-1)
        numer_sum = jnp.einsum('gts,sh->tgh', weights.astype(jnp.bfloat16).astype(jnp.float32), v_one.astype(jnp.float32))
        return numer_sum / jnp.transpose(denom_sum)[:, :, None]

    mapped = lax.map(one_group, (jnp.swapaxes(queries, 0, 1), jnp.swapaxes(key_rows, 0, 1), jnp.swapaxes(val_rows, 0, 1)))
    return jnp.swapaxes(mapped, 0, 1).astype(jnp.bfloat16)


def prefill_layer(x_res, layer_w):
    w_qkv, w_o, w_gate, w_up, w_down, g_attn, g_mlp = layer_w
    h_norm = rms_norm(x_res, g_attn)
    qkv_out = jnp.dot(h_norm, w_qkv.reshape(D, KV_HEADS * (GROUP + 2) * HEAD), preferred_element_type=jnp.float32)
    qkv_out = qkv_out.astype(jnp.bfloat16).reshape(TOKENS, KV_HEADS, GROUP + 2, HEAD)
    key_rows = qkv_out[:, :, GROUP]
    val_rows = qkv_out[:, :, GROUP + 1]
    attn_out = causal_attention(qkv_out[:, :, :GROUP], key_rows, val_rows)
    proj_out = jnp.dot(attn_out.reshape(TOKENS, HEADS * HEAD), w_o, preferred_element_type=jnp.float32)
    x_res = x_res + proj_out.astype(jnp.bfloat16)
    h_mlp = rms_norm(x_res, g_mlp)
    x_res = x_res + mlp_block(h_mlp, w_gate, w_up, w_down)
    return x_res, (key_rows, val_rows)


def decode_layer(y_res, operands):
    w_qkv, w_o, w_gate, w_up, w_down, g_attn, g_mlp, k_old, v_old = operands
    h_norm = rms_norm(y_res, g_attn)
    qkv_out = jnp.dot(h_norm[None], w_qkv.reshape(D, KV_HEADS * (GROUP + 2) * HEAD), preferred_element_type=jnp.float32)
    qkv_out = qkv_out.astype(jnp.bfloat16).reshape(KV_HEADS, GROUP + 2, HEAD).astype(jnp.float32)
    q_new = qkv_out[:, :GROUP]
    k_new = qkv_out[:, GROUP]
    v_new = qkv_out[:, GROUP + 1]
    attn_scale = HEAD ** -0.5
    s_old = jnp.einsum('kgh,tkh->kgt', q_new, k_old.astype(jnp.float32)) * attn_scale
    s_new = jnp.einsum('kgh,kh->kg', q_new, k_new) * attn_scale
    top_score = jnp.maximum(jnp.max(s_old, axis=-1), s_new)
    p_old = jnp.exp(s_old - top_score[:, :, None])
    p_new = jnp.exp(s_new - top_score)
    numer_sum = jnp.einsum('kgt,tkh->kgh', p_old.astype(jnp.bfloat16).astype(jnp.float32), v_old.astype(jnp.float32)) + p_new[:, :, None] * v_new[:, None, :]
    denom_sum = jnp.sum(p_old, axis=-1) + p_new
    attn_out = (numer_sum / denom_sum[:, :, None]).astype(jnp.bfloat16).reshape(1, HEADS * HEAD)
    proj_out = jnp.dot(attn_out, w_o, preferred_element_type=jnp.float32).astype(jnp.bfloat16)[0]
    y_res = y_res + proj_out.astype(jnp.float32)
    h_mlp = rms_norm(y_res, g_mlp)
    y_res = y_res + mlp_block(h_mlp[None], w_gate, w_up, w_down)[0].astype(jnp.float32)
    new_kv = jnp.stack([k_new, v_new]).astype(jnp.bfloat16)
    return y_res, new_kv


def reference(prompts, y_first, w_qkv, w_o, w_gate, w_up, w_down, g_attn, g_mlp):
    layers = (w_qkv, w_o, w_gate, w_up, w_down, g_attn, g_mlp)

    def prefill_one(x_req):
        return lax.scan(prefill_layer, x_req, layers)

    x_last, (k_all, v_all) = lax.map(prefill_one, prompts)
    k_cache = jnp.roll(k_all, 1, axis=0)
    v_cache = jnp.roll(v_all, 1, axis=0)

    def decode_one(operands):
        y_start, k_req, v_req = operands
        return lax.scan(decode_layer, y_start.astype(jnp.float32), layers + (k_req, v_req))

    y_last, kv_new = lax.map(decode_one, (y_first, k_cache, v_cache))
    return x_last, y_last, k_cache, v_cache, kv_new
```

```python
import functools

import jax
import jax.numpy as jnp
from jax import lax
from jax.experimental import pallas as pl
from jax.experimental.pallas import tpu as pltpu
from jax.sharding import PartitionSpec as P

NORM_EPS = 1e-5
MESH = pl.DeviceIdType.MESH
CHUNKS = 8
PAD = 16
COLS_A = 256
COLS_B = 512
LAGS = 6
F32 = jnp.float32
BF16 = jnp.bfloat16


def norm_rows(rows_f32, gain):
    inv_rms = lax.rsqrt(jnp.mean(rows_f32 * rows_f32, axis=-1, keepdims=True) + NORM_EPS)
    return (rows_f32 * inv_rms * gain).astype(BF16)


def remote(src, dst, send, recv, device):
    return pltpu.make_async_remote_copy(src_ref=src, dst_ref=dst, send_sem=send, recv_sem=recv, device_id=device, device_id_type=MESH)


def group_kernel(n_ho, n_tp, prompts, y_first, w_qkv, w_o, w_gate, w_up, w_down, gains, x_last, tail, kv_tok,
                 hid, part, pair_in, ring1, ring2, resid, kv, scores, qry, att, act, stage, wa, wb, cb0, cb1,
                 k_new, v_new, y_row, y_part, y_pair, y_chip, tail_out, tail_in,
                 wa_sem, wb_sem, in_sem, out_sem, pair_s, pair_r, r1_s, r1_r, r2_s, r2_r, a1_s, a1_r, a2_s, a2_r, d_s, d_r,
                 yp_s, yp_r, yc_s, yc_r, edge_s, edge_r, c0_s, c0_r, c1_s, c1_r, c2_s, c2_r, c2_l):
    tp = lax.axis_index("tp")
    ho = lax.axis_index("ho")
    n_chip = n_tp // 2
    core = lax.rem(tp, 2)
    chip = lax.div(tp, 2)
    to_right = {"tp": lax.rem(tp + 2, n_tp)}
    to_left = {"tp": lax.rem(tp + n_tp - 2, n_tp)}
    to_far = {"tp": lax.rem(tp + 4, n_tp)}
    to_pair = {"tp": tp + 1 - 2 * core}
    to_up = {"ho": lax.rem(ho + 1, n_ho)}
    to_down = {"ho": lax.rem(ho + n_ho - 1, n_ho)}
    c_right = lax.rem(chip + 1, n_chip)
    c_left = lax.rem(chip + n_chip - 1, n_chip)
    c_far = lax.rem(chip + 2, n_chip)

    n_layers, n_slots, d_model, head = w_qkv.shape
    n_group = n_slots - 2
    ff = w_gate.shape[2]
    n_tok = prompts.shape[1]
    rows = n_tok // CHUNKS
    half = rows // 2
    own = half // n_chip
    sub = own // 2
    all_rows = rows + PAD
    n_stage = 2 * n_layers
    n_steps = n_stage * CHUNKS
    t_qkv = n_slots * head // COLS_A
    t_gu = ff // COLS_A
    t_out = d_model // COLS_B
    mine = pl.multiple_of(core * half, half)
    theirs = pl.multiple_of(half - core * half, half)
    tok_dev = n_tok // n_tp
    tok_chip = 2 * tok_dev
    scale = head ** -0.5

    def block(base, which):
        return pl.multiple_of(base + which * own, own)

    barrier = pltpu.get_barrier_semaphore()
    peers = (to_right, to_left, to_far, to_pair, to_up, to_down)
    for peer in peers:
        pl.semaphore_signal(barrier, inc=1, device_id=peer, device_id_type=MESH)
    pl.semaphore_wait(barrier, len(peers))

    def qkv_copy(layer, t, u):
        return pltpu.make_async_copy(w_qkv.at[layer, t * 2 + u], wa.at[t, :, pl.ds(u * head, head)], wa_sem.at[t, u])

    def gu_copy(layer, t, u):
        slot = lax.rem(t, 2) * 2 + u
        cols = pl.ds(pl.multiple_of(t * COLS_A, COLS_A), COLS_A)
        return pltpu.make_async_copy((w_gate, w_up)[u].at[layer, :, cols], wa.at[slot], wa_sem.at[slot, 0])

    def out_copy(layer, t):
        slot = lax.rem(t, 3)
        cols = pl.ds(pl.multiple_of(t * COLS_B, COLS_B), COLS_B)
        return pltpu.make_async_copy(w_o.at[layer, :, cols], wb.at[slot, pl.ds(0, n_group * head)], wb_sem.at[slot])

    def down_copy(layer, t):
        slot = lax.rem(t, 3)
        cols = pl.ds(pl.multiple_of(t * COLS_B, COLS_B), COLS_B)
        return pltpu.make_async_copy(w_down.at[layer, :, cols], wb.at[slot], wb_sem.at[slot])

    def prompt_copy(c):
        return pltpu.make_async_copy(prompts.at[ho, pl.ds(pl.multiple_of(c * rows, rows), rows)], stage, in_sem)

    def prefetch(step):
        st = lax.div(step, CHUNKS)
        layer = lax.div(st, 2)

        @pl.when(st == 0)
        def _():
            prompt_copy(lax.rem(step, CHUNKS)).start()

        @pl.when(lax.rem(st, 2) == 0)
        def _():
            for t in range(t_qkv):
                for u in range(2):
                    qkv_copy(layer, t, u).start()
            for t in range(3):
                out_copy(layer, t).start()

        @pl.when(lax.rem(st, 2) == 1)
        def _():
            for t in range(2):
                for u in range(2):
                    gu_copy(layer, t, u).start()
            for t in range(3):
                down_copy(layer, t).start()

    def pair_copy(g):
        s = lax.rem(g, 2)
        return remote(part.at[lax.rem(g, 3), pl.ds(theirs, half)], pair_in.at[s], pair_s.at[s], pair_r.at[s], to_pair)

    def r1_copy(g, d):
        s = lax.rem(g, 2)
        base = pl.multiple_of(block(mine, c_far) + d * sub, sub)
        return remote(part.at[lax.rem(g, 3), pl.ds(base, sub)], ring1.at[s, d], r1_s.at[d], r1_r.at[s, d], (to_right, to_left)[d])

    def r2_copy(g, d):
        s = lax.rem(g, 2)
        base = block(mine, (c_right, c_left)[d])
        return remote(part.at[lax.rem(g, 3), pl.ds(base, own)], ring2.at[s, d], r2_s.at[d], r2_r.at[s, d], (to_right, to_left)[d])

    def a1_copy(g, d):
        c = lax.rem(g, CHUNKS)
        ref = hid.at[c, pl.ds(block(mine, chip), own)]
        return remote(ref, ref, a1_s.at[d], a1_r.at[c, d], (to_right, to_left)[d])

    def a2_copy(g, d):
        c = lax.rem(g, CHUNKS)
        base = pl.multiple_of(block(mine, (c_left, c_right)[d]) + d * sub, sub)
        ref = hid.at[c, pl.ds(base, sub)]
        return remote(ref, ref, a2_s.at[d], a2_r.at[c, d], (to_right, to_left)[d])

    def d_copy(g, i):
        c = lax.rem(g, CHUNKS)
        ref = hid.at[c, pl.ds(block(mine, (chip, c_left, c_right, c_far)[i]), own)]
        return remote(ref, ref, d_s.at[i], d_r.at[c, i], to_pair)

    def last_copy(c):
        return pltpu.make_async_copy(hid.at[c, pl.ds(0, rows)], x_last.at[pl.ds(pl.multiple_of(c * rows, rows), rows)], out_sem.at[c])

    def when_chunk(g, body):
        @pl.when(jnp.logical_and(g >= 0, g < n_steps))
        def _():
            body(g)

    def e1(g):
        pair_copy(g).wait_recv()
        pair_copy(g).wait_send()
        slot = lax.rem(g, 3)
        s = lax.rem(g, 2)

        @pl.loop(0, half // PAD)
        def _(i):
            dst = pl.ds(pl.multiple_of(mine + i * PAD, PAD), PAD)
            src = pl.ds(pl.multiple_of(i * PAD, PAD), PAD)
            part[slot, dst] = (part[slot, dst].astype(F32) + pair_in[s, src].astype(F32)).astype(BF16)

        for d in range(2):
            r1_copy(g, d).start()

    def e2(g):
        slot = lax.rem(g, 3)
        s = lax.rem(g, 2)
        for d in range(2):
            r1_copy(g, d).wait_send()
            r1_copy(g, d).wait_recv()
            dst = pl.ds(pl.multiple_of(block(mine, (c_right, c_left)[d]) + d * sub, sub), sub)
            part[slot, dst] = (part[slot, dst].astype(F32) + ring1[s, d].astype(F32)).astype(BF16)
            r2_copy(g, d).start()

    def e3(g):
        slot = lax.rem(g, 3)
        s = lax.rem(g, 2)
        c = lax.rem(g, CHUNKS)
        st = lax.div(g, CHUNKS)
        for d in range(2):
            r2_copy(g, d).wait_send()
            r2_copy(g, d).wait_recv()
        base = block(mine, chip)

        def new_rows(i):
            loc = pl.ds(i * PAD, PAD)
            dst = pl.ds(pl.multiple_of(base + i * PAD, PAD), PAD)
            total = part[slot, dst].astype(F32) + ring2[s, 0, loc].astype(F32) + ring2[s, 1, loc].astype(F32)
            return loc, dst, (resid[c, loc].astype(F32) + total.astype(BF16).astype(F32)).astype(BF16)

        @pl.when(st < n_stage - 1)
        def _():
            gain = gains[jnp.minimum(st + 1, n_stage - 1)]
            for i in range(own // PAD):
                loc, dst, new = new_rows(i)
                resid[c, loc] = new
                hid[c, dst] = norm_rows(new.astype(F32), gain)

        @pl.when(st == n_stage - 1)
        def _():
            for i in range(own // PAD):
                _, dst, new = new_rows(i)
                hid[c, dst] = new

        for d in range(2):
            a1_copy(g, d).start()
        d_copy(g, 0).start()

    def e4(g):
        for d in range(2):
            a1_copy(g, d).wait_send()
            a1_copy(g, d).wait_recv()
            a2_copy(g, d).start()
        d_copy(g, 0).wait_send()
        d_copy(g, 1).start()
        d_copy(g, 2).start()

    def e5(g):
        for d in range(2):
            a2_copy(g, d).wait_send()
            a2_copy(g, d).wait_recv()
        d_copy(g, 1).wait_send()
        d_copy(g, 2).wait_send()
        d_copy(g, 3).start()

    def e6(g):
        d_copy(g, 3).wait_send()
        for i in range(4):
            d_copy(g, i).wait_recv()

        @pl.when(g >= n_steps - CHUNKS)
        def _():
            last_copy(lax.rem(g, CHUNKS)).start()

    def y_pair_copy(st):
        return remote(y_part.at[st], y_pair.at[st], yp_s.at[st], yp_r.at[st], to_pair)

    def y_chip_copy(st, i):
        src_chip = chip
        return remote(y_chip.at[st, src_chip], y_chip.at[st, src_chip], yc_s.at[i], yc_r.at[st, i], (to_right, to_left, to_far)[i])

    first_copy = remote(y_first, y_row, edge_s.at[0], edge_r.at[0], to_down)
    tail_copy = remote(tail_out, tail_in, edge_s.at[1], edge_r.at[1], to_up)

    def put_y(gain):
        row = norm_rows(y_row[...], gain)
        hid[CHUNKS - 1, pl.ds(rows, PAD)] = jnp.broadcast_to(row.astype(F32), (PAD, d_model)).astype(BF16)

    def y_sum(st):
        y_pair_copy(st).wait_send()
        y_pair_copy(st).wait_recv()
        y_chip[st, chip] = y_part[st] + y_pair[st]
        for i in range(3):
            y_chip_copy(st, i).start()

    def y_done(st):
        for i in range(3):
            y_chip_copy(st, i).wait_send()
            y_chip_copy(st, i).wait_recv()
        total = y_chip[st, 0]
        for i in range(1, n_chip):
            total = total + y_chip[st, i]
        y_row[...] = y_row[...] + total.astype(BF16).astype(F32)

        @pl.when(st < n_stage - 1)
        def _():
            put_y(gains[jnp.minimum(st + 1, n_stage - 1)])

        @pl.when(st == n_stage - 1)
        def _():
            tail_out[:, pl.ds(0, d_model)] = y_row[...]
            tail_copy.start()

    def c0_copy(layer):
        return remote(kv.at[layer], cb0.at[layer], c0_s.at[layer], c0_r.at[layer], to_up)

    def c1_copy(layer, i):
        dst_chip = (c_right, c_left, c_far)[i]
        src = cb0.at[layer, :, pl.ds(pl.multiple_of(dst_chip * tok_chip, tok_chip), tok_chip)]
        return remote(src, cb1.at[layer, i], c1_s.at[layer, i], c1_r.at[layer, i], (to_right, to_left, to_far)[i])

    def c2_source(layer, i, which):
        off = pl.multiple_of(which * tok_dev, tok_dev)
        if i < 3:
            return cb1.at[layer, i, :, pl.ds(off, tok_dev)], (c_left, c_right, c_far)[i]
        return cb0.at[layer, :, pl.ds(pl.multiple_of(chip * tok_chip + off, tok_dev), tok_dev)], chip

    def c2_copy(layer, i):
        src, src_chip = c2_source(layer, i, 1 - core)
        return remote(src, kv_tok.at[layer, :, 2 * src_chip + core], c2_s.at[layer, i], c2_r.at[layer, i], to_pair)

    def c2_local(layer, i):
        src, src_chip = c2_source(layer, i, core)
        return pltpu.make_async_copy(src, kv_tok.at[layer, :, 2 * src_chip + core], c2_l.at[layer, i])

    def cache_events(g):
        for layer in range(n_layers):
            at = (2 * layer + 1) * CHUNKS

            @pl.when(g == at)
            def _():
                c0_copy(layer).start()

            @pl.when(g == at + 2)
            def _():
                c0_copy(layer).wait_send()
                c0_copy(layer).wait_recv()
                c1_copy(layer, 0).start()
                c1_copy(layer, 1).start()

            @pl.when(g == at + 3)
            def _():
                c1_copy(layer, 2).start()

            @pl.when(g == at + 5)
            def _():
                for i in range(3):
                    c1_copy(layer, i).wait_send()
                    c1_copy(layer, i).wait_recv()
                for i in range(4):
                    c2_copy(layer, i).start()
                    c2_local(layer, i).start()

            @pl.when(g == at + 7)
            def _():
                for i in range(4):
                    c2_copy(layer, i).wait_send()
                    c2_copy(layer, i).wait_recv()
                    c2_local(layer, i).wait()

    def store_part(g, t, acc):
        cols = pl.ds(pl.multiple_of(t * COLS_B, COLS_B), COLS_B)
        part[lax.rem(g, 3), :, cols] = acc[:rows].astype(BF16)
        y_part[lax.div(g, CHUNKS), :, cols] = acc[rows:rows + 1]

    def first_norm(c):
        prompt_copy(c).wait()
        gain = gains[0]

        @pl.loop(0, rows // PAD)
        def _(i):
            loc = pl.ds(pl.multiple_of(i * PAD, PAD), PAD)
            hid[c, loc] = norm_rows(stage[loc].astype(F32), gain)

        for i in range(own // PAD):
            resid[c, pl.ds(i * PAD, PAD)] = stage[pl.ds(pl.multiple_of(block(mine, chip) + i * PAD, PAD), PAD)]

        @pl.when(c == CHUNKS - 1)
        def _():
            first_copy.wait_send()
            first_copy.wait_recv()
            put_y(gain)

    def attention(layer, c):
        below = lax.broadcasted_iota(jnp.int32, (rows, rows), 0) - lax.broadcasted_iota(jnp.int32, (rows, rows), 1)
        for h in range(n_group):
            q = qry[pl.ds(0, rows), pl.ds(h * head, head)]

            def scores_of(j, top):
                loc = pl.ds(pl.multiple_of(j * rows, rows), rows)
                s = lax.dot_general(q, kv[layer, 0, loc], (((1,), (1,)), ((), ())), preferred_element_type=F32) * scale
                s = jnp.where(below >= (j - c) * rows, s, -jnp.inf)
                scores[:, loc] = s
                for b in range(rows // head):
                    top = jnp.maximum(top, s[:, b * head:(b + 1) * head])
                return top

            top = lax.fori_loop(0, c + 1, scores_of, jnp.full((rows, head), -jnp.inf, F32))
            top = jnp.max(top, axis=1, keepdims=True)

            def sums_of(j, carry):
                denom, numer = carry
                loc = pl.ds(pl.multiple_of(j * rows, rows), rows)
                p = jnp.exp(scores[:, loc] - top)
                for b in range(rows // head):
                    denom = denom + p[:, b * head:(b + 1) * head]
                return denom, numer + jnp.dot(p.astype(BF16), kv[layer, 1, loc], preferred_element_type=F32)

            zero = jnp.zeros((rows, head), F32)
            denom, numer = lax.fori_loop(0, c + 1, sums_of, (zero, zero))
            att[pl.ds(0, rows), pl.ds(h * head, head)] = (numer / jnp.sum(denom, axis=1, keepdims=True)).astype(BF16)

    def attention_new(layer):
        k_row = k_new[...].astype(F32)
        v_row = v_new[...].astype(F32)
        for h in range(n_group):
            q = qry[pl.ds(rows, PAD), pl.ds(h * head, head)]
            s_new = jnp.sum(q.astype(F32) * k_row, axis=1, keepdims=True) * scale

            def scores_of(j, top):
                loc = pl.ds(pl.multiple_of(j * rows, rows), rows)
                s = lax.dot_general(q, kv[layer, 0, loc], (((1,), (1,)), ((), ())), preferred_element_type=F32) * scale
                scores[pl.ds(0, PAD), loc] = s
                return jnp.maximum(top, jnp.max(s, axis=1, keepdims=True))

            top = lax.fori_loop(0, CHUNKS, scores_of, s_new)

            def sums_of(j, carry):
                denom, numer = carry
                loc = pl.ds(pl.multiple_of(j * rows, rows), rows)
                p = jnp.exp(scores[pl.ds(0, PAD), loc] - top)
                denom = denom + jnp.sum(p, axis=1, keepdims=True)
                return denom, numer + jnp.dot(p.astype(BF16), kv[layer, 1, loc], preferred_element_type=F32)

            p_new = jnp.exp(s_new - top)
            denom, numer = lax.fori_loop(0, CHUNKS, sums_of, (p_new, p_new * v_row))
            att[pl.ds(rows, PAD), pl.ds(h * head, head)] = (numer / denom).astype(BF16)

    def step_a(g, layer, c):
        @pl.when(layer == 0)
        def _():
            first_norm(c)

        for t in range(t_qkv):
            for u in range(2):
                qkv_copy(layer, t, u).wait()
            out = jnp.dot(hid[c], wa[t], preferred_element_type=F32).astype(BF16)
            if t < t_qkv - 1:
                qry[:, pl.ds(t * COLS_A, COLS_A)] = out
            else:
                loc = pl.ds(pl.multiple_of(c * rows, rows), rows)
                kv[layer, 0, loc] = out[:rows, :head]
                kv[layer, 1, loc] = out[:rows, head:]
                k_new[...] = out[rows:, :head]
                v_new[...] = out[rows:, head:]
        when_chunk(g - 1, e1)
        attention(layer, c)

        @pl.when(c == CHUNKS - 1)
        def _():
            attention_new(layer)
            for ll in range(n_layers):
                @pl.when(layer == ll)
                def _():
                    tail_out[:, pl.ds(d_model + 2 * ll * head, head)] = k_new[...].astype(F32)[:1]
                    tail_out[:, pl.ds(d_model + (2 * ll + 1) * head, head)] = v_new[...].astype(F32)[:1]

        @pl.loop(0, t_out)
        def _(t):
            out_copy(layer, t).wait()
            slot = lax.rem(t, 3)
            store_part(g, t, jnp.dot(att[...], wb[slot, :n_group * head], preferred_element_type=F32))

            @pl.when(t + 3 < t_out)
            def _():
                out_copy(layer, t + 3).start()

    def step_m(g, layer, c):
        @pl.loop(0, t_gu)
        def _(t):
            for u in range(2):
                gu_copy(layer, t, u).wait()
            slot = lax.rem(t, 2) * 2
            gate = jnp.dot(hid[c], wa[slot], preferred_element_type=F32)
            up = jnp.dot(hid[c], wa[slot + 1], preferred_element_type=F32)
            act[:, pl.ds(pl.multiple_of(t * COLS_A, COLS_A), COLS_A)] = (jax.nn.silu(gate) * up).astype(BF16)

            @pl.when(t + 2 < t_gu)
            def _():
                for u in range(2):
                    gu_copy(layer, t + 2, u).start()

        when_chunk(g - 1, e1)

        @pl.loop(0, t_out)
        def _(t):
            down_copy(layer, t).wait()
            slot = lax.rem(t, 3)
            store_part(g, t, jnp.dot(act[...], wb[slot], preferred_element_type=F32))

            @pl.when(t + 3 < t_out)
            def _():
                down_copy(layer, t + 3).start()

    first_copy.start()
    prefetch(0)
    for c in range(CHUNKS):
        hid[c, pl.ds(rows, PAD)] = jnp.zeros((PAD, d_model), BF16)

    @pl.loop(0, n_steps + LAGS)
    def _(g):
        st = lax.div(g, CHUNKS)
        c = lax.rem(g, CHUNKS)
        layer = lax.div(st, 2)
        when_chunk(g - 6, e6)
        when_chunk(g - 5, e5)
        when_chunk(g - 4, e4)
        when_chunk(g - 3, e3)
        when_chunk(g - 2, e2)

        @pl.when(jnp.logical_and(c == 0, jnp.logical_and(st >= 1, st <= n_stage)))
        def _():
            y_sum(st - 1)

        @pl.when(jnp.logical_and(c == 1, jnp.logical_and(st >= 1, st <= n_stage)))
        def _():
            y_done(st - 1)

        cache_events(g)

        @pl.when(jnp.logical_and(g < n_steps, lax.rem(st, 2) == 0))
        def _():
            step_a(g, layer, c)

        @pl.when(jnp.logical_and(g < n_steps, lax.rem(st, 2) == 1))
        def _():
            step_m(g, layer, c)

        @pl.when(g == n_steps)
        def _():
            e1(g - 1)

        @pl.when(g < n_steps)
        def _():
            pair_copy(g).start()

        @pl.when(jnp.logical_and(g < n_steps, c == CHUNKS - 1))
        def _():
            y_pair_copy(st).start()

        @pl.when(g + 1 < n_steps)
        def _():
            prefetch(g + 1)

    tail_copy.wait_send()
    tail_copy.wait_recv()
    tail[...] = tail_in[...]
    for c in range(CHUNKS):
        last_copy(c).wait()


def solution(mesh):
    n_ho, n_tp = mesh.shape['ho'], mesh.shape['tp']
    row_axes = ('pairs', 'ho')
    in_specs = (P('pairs', None, None), P(row_axes, None), P(None, None, 'tp', None, None), P(None, 'tp', None), P(None, None, 'tp'), P(None, None, 'tp'), P(None, 'tp', None), P(None, None), P(None, None))
    out_specs = (P(row_axes, None, None), P(row_axes, None), P(row_axes, None, 'tp', None, None), P(row_axes, None, 'tp', None, None), P(row_axes, None, None, 'tp', None))

    def device_program(prompts, y_first, w_qkv, w_o, w_gate, w_up, w_down, g_attn, g_mlp):
        n_layers, d_model, _, n_slots, head = w_qkv.shape
        n_tok = prompts.shape[1]
        ff = w_gate.shape[2]
        rows = n_tok // CHUNKS
        half = rows // 2
        own = half // (n_tp // 2)
        n_stage = 2 * n_layers
        group = n_slots - 2
        tok_dev = n_tok // n_tp
        wq = jnp.transpose(w_qkv[:, :, 0], (0, 2, 1, 3))
        gains = jnp.stack([g_attn, g_mlp], axis=1).reshape(n_stage, 1, d_model)
        tail_len = d_model + 2 * n_layers * head
        any_spec = pl.BlockSpec(memory_space=pl.ANY)
        vmem_spec = pl.BlockSpec(memory_space=pltpu.VMEM)
        dma = pltpu.SemaphoreType.DMA
        x_last, tail, kv_tok = pl.pallas_call(
            functools.partial(group_kernel, n_ho, n_tp),
            out_shape=(
                jax.ShapeDtypeStruct((n_tok, d_model), BF16),
                jax.ShapeDtypeStruct((1, tail_len), F32),
                jax.ShapeDtypeStruct((n_layers, 2, n_tp, tok_dev, head), BF16),
            ),
            in_specs=[any_spec, vmem_spec, any_spec, any_spec, any_spec, any_spec, any_spec, vmem_spec],
            out_specs=(any_spec, vmem_spec, any_spec),
            scratch_shapes=[
                pltpu.VMEM((CHUNKS, rows + PAD, d_model), BF16),
                pltpu.VMEM((3, rows, d_model), BF16),
                pltpu.VMEM((2, half, d_model), BF16),
                pltpu.VMEM((2, 2, own // 2, d_model), BF16),
                pltpu.VMEM((2, 2, own, d_model), BF16),
                pltpu.VMEM((CHUNKS, own, d_model), BF16),
                pltpu.VMEM((n_layers, 2, n_tok, head), BF16),
                pltpu.VMEM((rows, n_tok), F32),
                pltpu.VMEM((rows + PAD, group * head), BF16),
                pltpu.VMEM((rows + PAD, group * head), BF16),
                pltpu.VMEM((rows + PAD, ff), BF16),
                pltpu.VMEM((rows, d_model), BF16),
                pltpu.VMEM((4, d_model, COLS_A), BF16),
                pltpu.VMEM((3, ff, COLS_B), BF16),
                pltpu.VMEM((n_layers, 2, n_tok, head), BF16),
                pltpu.VMEM((n_layers, 3, 2, 2 * tok_dev, head), BF16),
                pltpu.VMEM((PAD, head), BF16),
                pltpu.VMEM((PAD, head), BF16),
                pltpu.VMEM((1, d_model), F32),
                pltpu.VMEM((n_stage, 1, d_model), F32),
                pltpu.VMEM((n_stage, 1, d_model), F32),
                pltpu.VMEM((n_stage, n_tp // 2, 1, d_model), F32),
                pltpu.VMEM((1, tail_len), F32),
                pltpu.VMEM((1, tail_len), F32),
                dma((4, 2)), dma((3,)), dma, dma((CHUNKS,)),
                dma((2,)), dma((2,)), dma((2,)), dma((2, 2)), dma((2,)), dma((2, 2)),
                dma((2,)), dma((CHUNKS, 2)), dma((2,)), dma((CHUNKS, 2)), dma((4,)), dma((CHUNKS, 4)),
                dma((n_stage,)), dma((n_stage,)), dma((3,)), dma((n_stage, 3)), dma((2,)), dma((2,)),
                dma((n_layers,)), dma((n_layers,)), dma((n_layers, 3)), dma((n_layers, 3)),
                dma((n_layers, 4)), dma((n_layers, 4)), dma((n_layers, 4)),
            ],
            compiler_params=pltpu.CompilerParams(collective_id=0, has_side_effects=True, vmem_limit_bytes=67043328),
            name="group_step",
        )(prompts, y_first.astype(F32), wq, w_o, w_gate, w_up, w_down, gains)
        y_last = tail[:, :d_model]
        kv_new = tail[:, d_model:].reshape(n_layers, 2, 1, head).astype(BF16)
        cache = jnp.transpose(kv_tok, (1, 0, 3, 2, 4))
        return x_last[None], y_last, cache[0][None], cache[1][None], kv_new[None]

    return jax.shard_map(device_program, mesh=mesh, in_specs=in_specs, out_specs=out_specs, check_vma=False)
```

```python
import functools

import jax
import jax.numpy as jnp
from jax import lax
from jax.experimental import pallas as pl
from jax.experimental.pallas import tpu as pltpu
from jax.sharding import PartitionSpec as P

NORM_EPS = 1e-5
MESH = pl.DeviceIdType.MESH
CHUNKS = 8
PAD = 16
COLS_A = 256
COLS_B = 1024
LAGS = 6
NORM_ROWS = 32
VMEM_LIMIT = 187 << 18
CONTRACT_LAST = (((1,), (1,)), ((), ()))
F32 = jnp.float32
BF16 = jnp.bfloat16


def norm_rows(rows_f32, gain):
    inv_rms = lax.rsqrt(jnp.mean(rows_f32 * rows_f32, axis=-1, keepdims=True) + NORM_EPS)
    return (rows_f32 * inv_rms * gain).astype(BF16)


def remote(src, dst, send, recv, device):
    return pltpu.make_async_remote_copy(src_ref=src, dst_ref=dst, send_sem=send, recv_sem=recv, device_id=device, device_id_type=MESH)


def group_kernel(n_ho, n_tp, prompts, y_first, w_qkv, w_o, w_gate, w_up, w_down, g_attn, g_mlp, hid, tail, k_tok, v_tok,
                 part, pair_in, ring1, ring2, resid, kv, scores, qry, att, act, wa, wb, cb0, cb1, relay,
                 k_new, v_new, gains, y_row, y_part, y_pair, y_chip, tail_out, tail_in,
                 wa_sem, wb_sem, in_sem, pair_s, pair_r, r1_s, r1_r, r2_s, r2_r, a1_s, a1_r, a2_s, a2_r, d_s, d_r,
                 yp_s, yp_r, yc_s, yc_r, edge_s, edge_r, c0_s, c0_r, c1_s, c1_r, c2_s, c2_r, c2_l):
    tp = lax.axis_index("tp")
    ho = lax.axis_index("ho")
    n_chip = n_tp // 2
    core = lax.rem(tp, 2)
    chip = lax.div(tp, 2)
    to_right = {"tp": lax.rem(tp + 2, n_tp)}
    to_left = {"tp": lax.rem(tp + n_tp - 2, n_tp)}
    to_far = {"tp": lax.rem(tp + 4, n_tp)}
    to_pair = {"tp": tp + 1 - 2 * core}
    to_up = {"ho": lax.rem(ho + 1, n_ho)}
    to_down = {"ho": lax.rem(ho + n_ho - 1, n_ho)}
    c_right = lax.rem(chip + 1, n_chip)
    c_left = lax.rem(chip + n_chip - 1, n_chip)
    c_far = lax.rem(chip + 2, n_chip)

    n_layers, n_slots, d_model, head = w_qkv.shape
    n_group = n_slots - 2
    ff = w_gate.shape[2]
    n_tok = prompts.shape[1]
    rows = n_tok // CHUNKS
    half = rows // 2
    own = half // n_chip
    sub = own // 2
    all_rows = rows + PAD
    n_stage = 2 * n_layers
    n_steps = n_stage * CHUNKS
    o_rows = n_group * head
    o_per_slot = ff // o_rows
    t_qkv = n_slots * head // COLS_A
    t_gu = ff // COLS_A
    t_out = d_model // COLS_B
    mine = pl.multiple_of(core * half, half)
    theirs = pl.multiple_of(half - core * half, half)
    tok_dev = n_tok // n_tp
    tok_chip = 2 * tok_dev
    scale = head ** -0.5

    def block(base, which):
        return pl.multiple_of(base + which * own, own)

    tail_out[:, pl.ds(0, d_model)] = y_first[...].astype(F32)
    barrier = pltpu.get_barrier_semaphore()
    peers = (to_right, to_left, to_far, to_pair, to_up, to_down)
    for peer in peers:
        pl.semaphore_signal(barrier, inc=1, device_id=peer, device_id_type=MESH)
    def qkv_copy(layer, t, u):
        return pltpu.make_async_copy(w_qkv.at[layer, t * 2 + u], wa.at[t, :, pl.ds(u * head, head)], wa_sem.at[t, u])

    def gu_copy(layer, t, u):
        slot = lax.rem(t, 2) * 2 + u
        cols = pl.ds(pl.multiple_of(t * COLS_A, COLS_A), COLS_A)
        return pltpu.make_async_copy((w_gate, w_up)[u].at[layer, :, cols], wa.at[slot], wa_sem.at[slot, 0])

    def out_tile(t):
        return wb.at[t // o_per_slot, pl.ds((t % o_per_slot) * o_rows, o_rows)]

    def out_copy(layer, t):
        return pltpu.make_async_copy(w_o.at[layer, :, pl.ds(t * COLS_B, COLS_B)], out_tile(t), wb_sem.at[t])

    def down_copy(layer, t):
        slot = lax.rem(t, 2)
        cols = pl.ds(pl.multiple_of(t * COLS_B, COLS_B), COLS_B)
        return pltpu.make_async_copy(w_down.at[layer, :, cols], wb.at[slot], wb_sem.at[slot])

    def prompt_copy(c):
        return pltpu.make_async_copy(prompts.at[ho, pl.ds(pl.multiple_of(c * rows, rows), rows)], hid.at[c, pl.ds(0, rows)], in_sem.at[c])

    def start_qkv(layer):
        for t in range(t_qkv):
            for u in range(2):
                qkv_copy(layer, t, u).start()

    def start_out(layer):
        for t in range(t_out):
            out_copy(layer, t).start()

    def start_gu(layer, t):
        for u in range(2):
            gu_copy(layer, t, u).start()

    def pair_copy(g):
        s = lax.rem(g, 2)
        return remote(part.at[lax.rem(g, 3), pl.ds(theirs, half)], pair_in.at[s], pair_s.at[s], pair_r.at[s], to_pair)

    def r1_copy(g, d):
        s = lax.rem(g, 2)
        base = pl.multiple_of(block(mine, c_far) + d * sub, sub)
        return remote(part.at[lax.rem(g, 3), pl.ds(base, sub)], ring1.at[s, d], r1_s.at[d], r1_r.at[s, d], (to_right, to_left)[d])

    def r2_copy(g, d):
        s = lax.rem(g, 2)
        base = block(mine, (c_right, c_left)[d])
        return remote(part.at[lax.rem(g, 3), pl.ds(base, own)], ring2.at[s, d], r2_s.at[d], r2_r.at[s, d], (to_right, to_left)[d])

    def a1_copy(g, d):
        c = lax.rem(g, CHUNKS)
        ref = hid.at[c, pl.ds(block(mine, chip), own)]
        return remote(ref, ref, a1_s.at[d], a1_r.at[c, d], (to_right, to_left)[d])

    def a2_copy(g, d):
        c = lax.rem(g, CHUNKS)
        base = pl.multiple_of(block(mine, (c_left, c_right)[d]) + d * sub, sub)
        ref = hid.at[c, pl.ds(base, sub)]
        return remote(ref, ref, a2_s.at[d], a2_r.at[c, d], (to_right, to_left)[d])

    def d_copy(g, i):
        c = lax.rem(g, CHUNKS)
        ref = hid.at[c, pl.ds(block(mine, (chip, c_left, c_right, c_far)[i]), own)]
        return remote(ref, ref, d_s.at[i], d_r.at[c, i], to_pair)

    def when_chunk(g, body):
        @pl.when(jnp.logical_and(g >= 0, g < n_steps))
        def _():
            body(g)

    def e1(g):
        pair_copy(g).wait_recv()
        pair_copy(g).wait_send()
        slot = lax.rem(g, 3)
        s = lax.rem(g, 2)

        @pl.loop(0, half // PAD)
        def _(i):
            dst = pl.ds(pl.multiple_of(mine + i * PAD, PAD), PAD)
            src = pl.ds(pl.multiple_of(i * PAD, PAD), PAD)
            part[slot, dst] = (part[slot, dst].astype(F32) + pair_in[s, src].astype(F32)).astype(BF16)

        for d in range(2):
            r1_copy(g, d).start()

    def e2(g):
        slot = lax.rem(g, 3)
        s = lax.rem(g, 2)
        for d in range(2):
            r1_copy(g, d).wait_send()
            r1_copy(g, d).wait_recv()
            dst = pl.ds(pl.multiple_of(block(mine, (c_right, c_left)[d]) + d * sub, sub), sub)
            part[slot, dst] = (part[slot, dst].astype(F32) + ring1[s, d].astype(F32)).astype(BF16)
            r2_copy(g, d).start()

    def e3(g):
        slot = lax.rem(g, 3)
        s = lax.rem(g, 2)
        c = lax.rem(g, CHUNKS)
        st = lax.div(g, CHUNKS)
        for d in range(2):
            r2_copy(g, d).wait_send()
            r2_copy(g, d).wait_recv()
        base = block(mine, chip)

        def new_rows(i):
            loc = pl.ds(i * PAD, PAD)
            dst = pl.ds(pl.multiple_of(base + i * PAD, PAD), PAD)
            total = part[slot, dst].astype(F32) + ring2[s, 0, loc].astype(F32) + ring2[s, 1, loc].astype(F32)
            return loc, dst, (resid[c, loc].astype(F32) + total.astype(BF16).astype(F32)).astype(BF16)

        @pl.when(st < n_stage - 1)
        def _():
            gain = gains[jnp.minimum(st + 1, n_stage - 1)]
            for i in range(own // PAD):
                loc, dst, new = new_rows(i)
                resid[c, loc] = new
                hid[c, dst] = norm_rows(new.astype(F32), gain)

        @pl.when(st == n_stage - 1)
        def _():
            for i in range(own // PAD):
                _, dst, new = new_rows(i)
                hid[c, dst] = new

        for d in range(2):
            a1_copy(g, d).start()
        d_copy(g, 0).start()

    def e4(g):
        for d in range(2):
            a1_copy(g, d).wait_send()
            a1_copy(g, d).wait_recv()
            a2_copy(g, d).start()
        d_copy(g, 0).wait_send()
        d_copy(g, 1).start()
        d_copy(g, 2).start()

    def e5(g):
        for d in range(2):
            a2_copy(g, d).wait_send()
            a2_copy(g, d).wait_recv()
        d_copy(g, 1).wait_send()
        d_copy(g, 2).wait_send()
        d_copy(g, 3).start()

    def e6(g):
        d_copy(g, 3).wait_send()
        for i in range(4):
            d_copy(g, i).wait_recv()

    def y_pair_copy(st):
        return remote(y_part.at[st], y_pair.at[st], yp_s.at[st], yp_r.at[st], to_pair)

    def y_chip_copy(st, i):
        src_chip = chip
        return remote(y_chip.at[st, src_chip], y_chip.at[st, src_chip], yc_s.at[i], yc_r.at[st, i], (to_right, to_left, to_far)[i])

    first_copy = remote(tail_out.at[:, pl.ds(0, d_model)], y_row, edge_s.at[0], edge_r.at[0], to_down)
    tail_copy = remote(tail_out, tail_in, edge_s.at[1], edge_r.at[1], to_up)

    def put_y(gain):
        row = norm_rows(y_row[...], gain)
        hid[CHUNKS - 1, pl.ds(rows, PAD)] = jnp.broadcast_to(row.astype(F32), (PAD, d_model)).astype(BF16)

    def y_sum(st):
        y_pair_copy(st).wait_send()
        y_pair_copy(st).wait_recv()
        y_chip[st, chip] = y_part[st] + y_pair[st]
        for i in range(3):
            y_chip_copy(st, i).start()

    def y_done(st):
        for i in range(3):
            y_chip_copy(st, i).wait_send()
            y_chip_copy(st, i).wait_recv()
        total = y_chip[st, 0]
        for i in range(1, n_chip):
            total = total + y_chip[st, i]
        y_row[...] = y_row[...] + total.astype(BF16).astype(F32)

        @pl.when(st < n_stage - 1)
        def _():
            put_y(gains[jnp.minimum(st + 1, n_stage - 1)])

        @pl.when(st == n_stage - 1)
        def _():
            tail_out[:, pl.ds(0, d_model)] = y_row[...]
            tail_copy.start()

    def c0_copy(layer):
        return remote(kv.at[layer], cb0.at[layer], c0_s.at[layer], c0_r.at[layer], to_up)

    def c1_copy(layer, i):
        def tokens(c):
            return pl.ds(pl.multiple_of(c * tok_chip, tok_chip), tok_chip)

        src, dst, to = (
            (cb0.at[layer, :, tokens(c_right)], cb1.at[layer, 0], to_right),
            (cb0.at[layer, :, tokens(c_left)], cb1.at[layer, 1], to_left),
            (cb0.at[layer, 0, tokens(c_far)], relay.at[layer, 0], to_right),
            (cb0.at[layer, 1, tokens(c_far)], relay.at[layer, 1], to_left),
            (relay.at[layer, 0], cb1.at[layer, 2, 0], to_right),
            (relay.at[layer, 1], cb1.at[layer, 2, 1], to_left),
        )[i]
        return remote(src, dst, c1_s.at[layer, i], c1_r.at[layer, i], to)

    def c2_source(layer, i, n, which):
        off = pl.multiple_of(which * tok_dev, tok_dev)
        if i < 3:
            return cb1.at[layer, i, n, pl.ds(off, tok_dev)], (c_left, c_right, c_far)[i]
        return cb0.at[layer, n, pl.ds(pl.multiple_of(chip * tok_chip + off, tok_dev), tok_dev)], chip

    def c2_copy(layer, i, n):
        src, src_chip = c2_source(layer, i, n, 1 - core)
        return remote(src, (k_tok, v_tok)[n].at[layer, 2 * src_chip + core], c2_s.at[layer, i, n], c2_r.at[layer, i, n], to_pair)

    def c2_local(layer, i, n):
        src, src_chip = c2_source(layer, i, n, core)
        return pltpu.make_async_copy(src, (k_tok, v_tok)[n].at[layer, 2 * src_chip + core], c2_l.at[layer, i, n])

    def cache_events(g):
        for layer in range(n_layers):
            at = (2 * layer + 1) * CHUNKS

            @pl.when(g == at)
            def _():
                c0_copy(layer).start()

            @pl.when(g == at + 2)
            def _():
                c0_copy(layer).wait_send()
                c0_copy(layer).wait_recv()
                c1_copy(layer, 0).start()
                c1_copy(layer, 1).start()

            @pl.when(g == at + 3)
            def _():
                c1_copy(layer, 2).start()
                c1_copy(layer, 3).start()

            @pl.when(g == at + 5)
            def _():
                for i in (2, 3):
                    c1_copy(layer, i).wait_send()
                    c1_copy(layer, i).wait_recv()
                for i in (4, 5):
                    c1_copy(layer, i).start()

            @pl.when(g == at + 7)
            def _():
                for i in (0, 1, 4, 5):
                    c1_copy(layer, i).wait_send()
                    c1_copy(layer, i).wait_recv()
                for i in range(4):
                    for n in range(2):
                        c2_copy(layer, i, n).start()
                        c2_local(layer, i, n).start()

            @pl.when(g == at + 9)
            def _():
                for i in range(4):
                    for n in range(2):
                        c2_copy(layer, i, n).wait_send()
                        c2_copy(layer, i, n).wait_recv()
                        c2_local(layer, i, n).wait()

    def store_part(g, t, acc):
        cols = pl.ds(pl.multiple_of(t * COLS_B, COLS_B), COLS_B)
        part[lax.rem(g, 3), :, cols] = acc[:rows].astype(BF16)
        y_part[lax.div(g, CHUNKS), :, cols] = acc[rows:rows + 1]

    def first_norm(c):
        prompt_copy(c).wait()
        gain = gains[0]
        for i in range(own // PAD):
            resid[c, pl.ds(i * PAD, PAD)] = hid[c, pl.ds(pl.multiple_of(block(mine, chip) + i * PAD, PAD), PAD)]

        @pl.loop(0, rows // NORM_ROWS)
        def _(i):
            loc = pl.ds(pl.multiple_of(i * NORM_ROWS, NORM_ROWS), NORM_ROWS)
            hid[c, loc] = norm_rows(hid[c, loc].astype(F32), gain)

        @pl.when(c == CHUNKS - 1)
        def _():
            first_copy.wait_send()
            first_copy.wait_recv()
            put_y(gain)

    def attention(layer, c):
        causal = lax.broadcasted_iota(jnp.int32, (rows, rows), 0) >= lax.broadcasted_iota(jnp.int32, (rows, rows), 1)
        heads = range(n_group)

        def loc_of(j):
            return pl.ds(pl.multiple_of(j * rows, rows), rows)

        def score(h, loc):
            q = qry[pl.ds(0, rows), pl.ds(h * head, head)]
            return lax.dot_general(q, kv[layer, 0, loc], CONTRACT_LAST, preferred_element_type=F32) * scale

        def fold(op, x, s):
            for b in range(rows // head):
                x = op(x, s[:, b * head:(b + 1) * head])
            return x

        def first(j, tops):
            loc = loc_of(j)
            new = []
            for h in heads:
                s = score(h, loc)
                scores[h, :, loc] = s
                new.append(fold(jnp.maximum, tops[h], s))
            return tuple(new)

        lowest = jnp.full((rows, head), -jnp.inf, F32)
        tops = lax.fori_loop(0, c, first, tuple(lowest for _ in heads))
        diag = loc_of(c)
        row_top = []
        for h in heads:
            s = jnp.where(causal, score(h, diag), -jnp.inf)
            scores[h, :, diag] = s
            row_top.append(jnp.max(fold(jnp.maximum, tops[h], s), axis=1, keepdims=True))

        def second(j, carry):
            loc = loc_of(j)
            new = []
            for h in heads:
                denom, numer = carry[h]
                p = jnp.exp(scores[h, :, loc] - row_top[h])
                new.append((fold(jnp.add, denom, p), numer + jnp.dot(p.astype(BF16), kv[layer, 1, loc], preferred_element_type=F32)))
            return tuple(new)

        zero = jnp.zeros((rows, head), F32)
        sums = lax.fori_loop(0, c + 1, second, tuple((zero, zero) for _ in heads))
        for h in heads:
            denom, numer = sums[h]
            att[pl.ds(0, rows), pl.ds(h * head, head)] = (numer / jnp.sum(denom, axis=1, keepdims=True)).astype(BF16)

    def attention_new(layer):
        q = jnp.concatenate([qry[pl.ds(rows, PAD), pl.ds(h * head, head)] for h in range(n_group)], axis=0)
        k_row = k_new[...].astype(F32)[:1]
        v_row = v_new[...].astype(F32)[:1]
        s_new = jnp.sum(q.astype(F32) * k_row, axis=1, keepdims=True) * scale
        s_old = lax.dot_general(q, kv[layer, 0], CONTRACT_LAST, preferred_element_type=F32) * scale
        top = jnp.maximum(jnp.max(s_old, axis=1, keepdims=True), s_new)
        p_old = jnp.exp(s_old - top)
        p_new = jnp.exp(s_new - top)
        denom = jnp.sum(p_old, axis=1, keepdims=True) + p_new
        numer = jnp.dot(p_old.astype(BF16), kv[layer, 1], preferred_element_type=F32) + p_new * v_row
        out = (numer / denom).astype(BF16)
        for h in range(n_group):
            att[pl.ds(rows, PAD), pl.ds(h * head, head)] = out[h * PAD:(h + 1) * PAD]

    def step_a(g, layer, c):
        @pl.when(layer == 0)
        def _():
            first_norm(c)

        @pl.when(c == 0)
        def _():
            for t in range(t_qkv):
                for u in range(2):
                    qkv_copy(layer, t, u).wait()

        for t in range(t_qkv):
            out = jnp.dot(hid[c], wa[t], preferred_element_type=F32).astype(BF16)
            if t < t_qkv - 1:
                qry[:, pl.ds(t * COLS_A, COLS_A)] = out
            else:
                loc = pl.ds(pl.multiple_of(c * rows, rows), rows)
                kv[layer, 0, loc] = out[:rows, :head]
                kv[layer, 1, loc] = out[:rows, head:]
                k_new[...] = out[rows:, :head]
                v_new[...] = out[rows:, head:]

        @pl.when(c == CHUNKS - 1)
        def _():
            for t in range(2):
                start_gu(layer, t)

        when_chunk(g - 1, e1)
        attention(layer, c)

        @pl.when(c == CHUNKS - 1)
        def _():
            attention_new(layer)
            for ll in range(n_layers):
                @pl.when(layer == ll)
                def _():
                    tail_out[:, pl.ds(d_model + 2 * ll * head, head)] = k_new[...].astype(F32)[:1]
                    tail_out[:, pl.ds(d_model + (2 * ll + 1) * head, head)] = v_new[...].astype(F32)[:1]

        @pl.when(c == 0)
        def _():
            for t in range(t_out):
                out_copy(layer, t).wait()

        for t in range(t_out):
            store_part(g, t, jnp.dot(att[...], out_tile(t)[...], preferred_element_type=F32))

        @pl.when(c == CHUNKS - 1)
        def _():
            for t in range(2):
                down_copy(layer, t).start()

    def step_m(g, layer, c):
        @pl.loop(0, t_gu)
        def _(t):
            for u in range(2):
                gu_copy(layer, t, u).wait()
            slot = lax.rem(t, 2) * 2
            gate = jnp.dot(hid[c], wa[slot], preferred_element_type=F32)
            up = jnp.dot(hid[c], wa[slot + 1], preferred_element_type=F32)
            act[:, pl.ds(pl.multiple_of(t * COLS_A, COLS_A), COLS_A)] = (jax.nn.silu(gate) * up).astype(BF16)

            @pl.when(jnp.logical_or(t + 2 < t_gu, c + 1 < CHUNKS))
            def _():
                start_gu(layer, lax.rem(t + 2, t_gu))

        @pl.when(jnp.logical_and(c == CHUNKS - 1, layer + 1 < n_layers))
        def _():
            start_qkv(jnp.minimum(layer + 1, n_layers - 1))

        when_chunk(g - 1, e1)

        @pl.loop(0, t_out)
        def _(t):
            down_copy(layer, t).wait()
            store_part(g, t, jnp.dot(act[...], wb[lax.rem(t, 2)], preferred_element_type=F32))

            @pl.when(jnp.logical_or(t + 2 < t_out, c + 1 < CHUNKS))
            def _():
                down_copy(layer, lax.rem(t + 2, t_out)).start()

        @pl.when(jnp.logical_and(c == CHUNKS - 1, layer + 1 < n_layers))
        def _():
            start_out(jnp.minimum(layer + 1, n_layers - 1))

    start_qkv(0)
    prompt_copy(0).start()
    start_out(0)
    for c in range(1, CHUNKS):
        prompt_copy(c).start()
    for layer in range(n_layers):
        gains[2 * layer] = g_attn[layer:layer + 1]
        gains[2 * layer + 1] = g_mlp[layer:layer + 1]
    for c in range(CHUNKS):
        hid[c, pl.ds(rows, PAD)] = jnp.zeros((PAD, d_model), BF16)
    att[pl.ds(rows, PAD)] = jnp.zeros((PAD, o_rows), BF16)
    pl.semaphore_wait(barrier, len(peers))
    first_copy.start()

    @pl.loop(0, n_steps + LAGS)
    def _(g):
        st = lax.div(g, CHUNKS)
        c = lax.rem(g, CHUNKS)
        layer = lax.div(st, 2)
        when_chunk(g - 6, e6)
        when_chunk(g - 5, e5)
        when_chunk(g - 4, e4)
        when_chunk(g - 3, e3)
        when_chunk(g - 2, e2)

        @pl.when(jnp.logical_and(c == 0, jnp.logical_and(st >= 1, st <= n_stage)))
        def _():
            y_sum(st - 1)

        @pl.when(jnp.logical_and(c == 1, jnp.logical_and(st >= 1, st <= n_stage)))
        def _():
            y_done(st - 1)

        cache_events(g)

        @pl.when(jnp.logical_and(g < n_steps, lax.rem(st, 2) == 0))
        def _():
            step_a(g, layer, c)

        @pl.when(jnp.logical_and(g < n_steps, lax.rem(st, 2) == 1))
        def _():
            step_m(g, layer, c)

        @pl.when(g == n_steps)
        def _():
            e1(g - 1)

        @pl.when(g < n_steps)
        def _():
            pair_copy(g).start()

        @pl.when(jnp.logical_and(g < n_steps, c == CHUNKS - 1))
        def _():
            y_pair_copy(st).start()

    tail_copy.wait_send()
    tail_copy.wait_recv()
    tail[...] = tail_in[...]


def solution(mesh):
    n_ho, n_tp = mesh.shape['ho'], mesh.shape['tp']
    row_axes = ('pairs', 'ho')
    in_specs = (P('pairs', None, None), P(row_axes, None), P(None, None, 'tp', None, None), P(None, 'tp', None), P(None, None, 'tp'), P(None, None, 'tp'), P(None, 'tp', None), P(None, None), P(None, None))
    out_specs = (P(row_axes, None, None), P(row_axes, None), P(row_axes, None, 'tp', None, None), P(row_axes, None, 'tp', None, None), P(row_axes, None, None, 'tp', None))

    def device_program(prompts, y_first, w_qkv, w_o, w_gate, w_up, w_down, g_attn, g_mlp):
        n_layers, d_model, _, n_slots, head = w_qkv.shape
        n_tok = prompts.shape[1]
        ff = w_gate.shape[2]
        rows = n_tok // CHUNKS
        half = rows // 2
        own = half // (n_tp // 2)
        n_stage = 2 * n_layers
        group = n_slots - 2
        tok_dev = n_tok // n_tp
        wq = jnp.transpose(w_qkv[:, :, 0], (0, 2, 1, 3))
        tail_len = d_model + 2 * n_layers * head
        any_spec = pl.BlockSpec(memory_space=pl.ANY)
        vmem_spec = pl.BlockSpec(memory_space=pltpu.VMEM)
        dma = pltpu.SemaphoreType.DMA
        hid, tail, k_tok, v_tok = pl.pallas_call(
            functools.partial(group_kernel, n_ho, n_tp),
            out_shape=(
                pltpu.VMEM((CHUNKS, rows + PAD, d_model), BF16),
                jax.ShapeDtypeStruct((1, tail_len), F32),
                jax.ShapeDtypeStruct((n_layers, n_tp, tok_dev, head), BF16),
                jax.ShapeDtypeStruct((n_layers, n_tp, tok_dev, head), BF16),
            ),
            in_specs=[any_spec, vmem_spec, any_spec, any_spec, any_spec, any_spec, any_spec, vmem_spec, vmem_spec],
            out_specs=(vmem_spec, vmem_spec, any_spec, any_spec),
            scratch_shapes=[
                pltpu.VMEM((3, rows, d_model), BF16),
                pltpu.VMEM((2, half, d_model), BF16),
                pltpu.VMEM((2, 2, own // 2, d_model), BF16),
                pltpu.VMEM((2, 2, own, d_model), BF16),
                pltpu.VMEM((CHUNKS, own, d_model), BF16),
                pltpu.VMEM((n_layers, 2, n_tok, head), BF16),
                pltpu.VMEM((group, rows, n_tok), F32),
                pltpu.VMEM((rows + PAD, group * head), BF16),
                pltpu.VMEM((rows + PAD, group * head), BF16),
                pltpu.VMEM((rows + PAD, ff), BF16),
                pltpu.VMEM((4, d_model, COLS_A), BF16),
                pltpu.VMEM((2, ff, COLS_B), BF16),
                pltpu.VMEM((n_layers, 2, n_tok, head), BF16),
                pltpu.VMEM((n_layers, 3, 2, 2 * tok_dev, head), BF16),
                pltpu.VMEM((n_layers, 2, 2 * tok_dev, head), BF16),
                pltpu.VMEM((PAD, head), BF16),
                pltpu.VMEM((PAD, head), BF16),
                pltpu.VMEM((n_stage, 1, d_model), F32),
                pltpu.VMEM((1, d_model), F32),
                pltpu.VMEM((n_stage, 1, d_model), F32),
                pltpu.VMEM((n_stage, 1, d_model), F32),
                pltpu.VMEM((n_stage, n_tp // 2, 1, d_model), F32),
                pltpu.VMEM((1, tail_len), F32),
                pltpu.VMEM((1, tail_len), F32),
                dma((4, 2)), dma((d_model // COLS_B,)), dma((CHUNKS,)),
                dma((2,)), dma((2,)), dma((2,)), dma((2, 2)), dma((2,)), dma((2, 2)),
                dma((2,)), dma((CHUNKS, 2)), dma((2,)), dma((CHUNKS, 2)), dma((4,)), dma((CHUNKS, 4)),
                dma((n_stage,)), dma((n_stage,)), dma((3,)), dma((n_stage, 3)), dma((2,)), dma((2,)),
                dma((n_layers,)), dma((n_layers,)), dma((n_layers, 6)), dma((n_layers, 6)),
                dma((n_layers, 4, 2)), dma((n_layers, 4, 2)), dma((n_layers, 4, 2)),
            ],
            compiler_params=pltpu.CompilerParams(collective_id=0, has_side_effects=True, vmem_limit_bytes=VMEM_LIMIT),
            name="group_step",
        )(prompts, y_first, wq, w_o, w_gate, w_up, w_down, g_attn, g_mlp)
        y_last = tail[:, :d_model]
        kv_new = tail[:, d_model:].reshape(n_layers, 2, 1, head).astype(BF16)
        x_last = hid[:, :rows].reshape(n_tok, d_model)
        k_cache, v_cache = jnp.swapaxes(k_tok, 1, 2), jnp.swapaxes(v_tok, 1, 2)
        return x_last[None], y_last, k_cache[None], v_cache[None], kv_new[None]

    return jax.shard_map(device_program, mesh=mesh, in_specs=in_specs, out_specs=out_specs, check_vma=False)
```

```python
import functools

import jax
import jax.numpy as jnp
from jax import lax
from jax.experimental import pallas as pl
from jax.experimental.pallas import tpu as pltpu
from jax.sharding import PartitionSpec as P

NORM_EPS = 1e-5
MESH = pl.DeviceIdType.MESH
CHUNKS = 8
PAD = 16
COLS_A = 256
COLS_B = 1024
LAGS = 6
NORM_ROWS = 32
VMEM_LIMIT = 46 << 20
WX_STEPS = (0, 0, 1, 2, 10, 11, 11, 12, 12, 13)
CACHE_STEPS = ((8, 16, 18, 20, 22, 24), (24, 26, 27, 29, 31, 33))
SLOTS_B = 3
CONTRACT_LAST = (((1,), (1,)), ((), ()))
F32 = jnp.float32
BF16 = jnp.bfloat16


def norm_rows(rows_f32, gain):
    inv_rms = lax.rsqrt(jnp.mean(rows_f32 * rows_f32, axis=-1, keepdims=True) + NORM_EPS)
    return (rows_f32 * inv_rms * gain).astype(BF16)


def remote(src, dst, send, recv, device):
    return pltpu.make_async_remote_copy(src_ref=src, dst_ref=dst, send_sem=send, recv_sem=recv, device_id=device, device_id_type=MESH)


def chip_group(chip):
    return lax.rem(lax.div(chip + 1, 2) + 1, 2)


def chip_member(chip):
    return lax.div(chip, 2)


def group_kernel(n_ho, n_tp, prompts, y_first, w_qkv, w_o, w_gate, w_up, w_down, g_attn, g_mlp, hid, tail, k_tok, v_tok, wq_x, wo_x, cb0, cb1, relay,
                 part, pair_in, ring1, ring2, resid, kv0, kv1, scores, qry, qry_new, att0, att1, act, wa, wb,
                 k_new, v_new, gains, y_row, y_part, y_pair, y_chip, tail_out, tail_in,
                 wa_sem, wb_sem, in_sem, pair_s, pair_r, r1_s, r1_r, r2_s, r2_r, a1_s, a1_r, a2_s, a2_r, d_s, d_r,
                 yp_s, yp_r, yc_s, yc_r, edge_s, edge_r, c0_s, c0_r, c1_s, c1_r, c2_s, c2_r, c2_l, kx_s, kx_r, wx_s, wx_r, wy_s, wy_r):
    tp = lax.axis_index("tp")
    ho = lax.axis_index("ho")
    n_chip = n_tp // 2
    core = lax.rem(tp, 2)
    chip = lax.div(tp, 2)
    odd = lax.rem(chip, 2)
    to_right = {"tp": lax.rem(tp + 2, n_tp)}
    to_left = {"tp": lax.rem(tp + n_tp - 2, n_tp)}
    to_far = {"tp": lax.rem(tp + 4, n_tp)}
    to_pair = {"tp": tp + 1 - 2 * core}
    to_up = {"ho": lax.rem(ho + 1, n_ho)}
    to_down = {"ho": lax.rem(ho + n_ho - 1, n_ho)}
    c_right = lax.rem(chip + 1, n_chip)
    c_left = lax.rem(chip + n_chip - 1, n_chip)
    c_far = lax.rem(chip + 2, n_chip)
    c_mate = lax.rem(chip + n_chip + 2 * odd - 1, n_chip)
    to_mate = {"tp": lax.rem(tp + n_tp + 4 * odd - 2, n_tp)}
    to_swap = {"tp": lax.rem(tp + n_tp + 2 - 4 * odd, n_tp)}
    mate_out = 1 - odd
    mate_in = odd
    grp = chip_group(chip)

    n_layers, n_slots, d_model, head = w_qkv.shape
    n_group = n_slots - 2
    ff = w_gate.shape[2]
    n_tok = prompts.shape[1]
    rows = n_tok // CHUNKS
    half = rows // 2
    seg = half // 2
    own = half // n_chip
    sub = own // 2
    n_stage = 2 * n_layers
    n_steps = n_stage * CHUNKS
    swap_stage = n_stage - 2
    swap_layer = n_layers - 1
    o_rows = n_group * head
    o_per_slot = ff // o_rows
    t_qkv = n_slots * head // COLS_A
    t_gu = ff // COLS_A
    t_out = d_model // COLS_B
    tok_dev = n_tok // n_tp
    tok_chip = 2 * tok_dev
    scale = head ** -0.5

    def block_row(c, k):
        return pl.multiple_of(chip_group(c) * half + k * seg + chip_member(c) * own, own)

    def part_block(g, c, first, size):
        return part.at[lax.rem(g, 3), chip_group(c), core, pl.ds(pl.multiple_of(chip_member(c) * own + first, size), size)]

    tail_out[:, pl.ds(0, d_model)] = y_first[...].astype(F32)
    barrier = pltpu.get_barrier_semaphore()
    peers = (to_right, to_left, to_far, to_pair, to_up, to_down)
    for peer in peers:
        pl.semaphore_signal(barrier, inc=1, device_id=peer, device_id_type=MESH)

    def qkv_copy(layer, t, u):
        return pltpu.make_async_copy(w_qkv.at[layer, t * 2 + u], wa.at[t, :, pl.ds(u * head, head)], wa_sem.at[t, u])

    def swap_qkv_copy(slot, t, u):
        src = w_qkv.at[swap_layer, t * 2 + u] if t < t_qkv else wq_x.at[(t - t_qkv) * 2 + u]
        return pltpu.make_async_copy(src, wa.at[slot, :, pl.ds(u * head, head)], wa_sem.at[slot, u])

    def start_swap_qkv(c, pair):
        slot = lax.rem(c * t_qkv + pair, 2) * 2
        for v in range(2):
            for u in range(2):
                swap_qkv_copy(slot + v, 2 * pair + v, u).start()

    def gu_copy(layer, t, u):
        slot = lax.rem(t, 2) * 2 + u
        cols = pl.ds(pl.multiple_of(t * COLS_A, COLS_A), COLS_A)
        return pltpu.make_async_copy((w_gate, w_up)[u].at[layer, :, cols], wa.at[slot], wa_sem.at[slot, 0])

    def out_tile(t):
        return wb.at[t // o_per_slot, pl.ds((t % o_per_slot) * o_rows, o_rows)]

    def out_copy(layer, t):
        return pltpu.make_async_copy(w_o.at[layer, :, pl.ds(t * COLS_B, COLS_B)], out_tile(t), wb_sem.at[t])

    def swap_out_copy(c, t, v):
        slot = lax.rem(c * t_out + t, SLOTS_B)
        src = (w_o.at[swap_layer], wo_x)[v].at[:, pl.ds(t * COLS_B, COLS_B)]
        return pltpu.make_async_copy(src, wb.at[slot, pl.ds(v * o_rows, o_rows)], wb_sem.at[slot * 2 + v])

    def down_copy(layer, c, t):
        slot = lax.rem(c * t_out + t, SLOTS_B)
        cols = pl.ds(pl.multiple_of(t * COLS_B, COLS_B), COLS_B)
        return pltpu.make_async_copy(w_down.at[layer, :, cols], wb.at[slot], wb_sem.at[slot])

    def prompt_copy(c):
        return pltpu.make_async_copy(prompts.at[ho, pl.ds(pl.multiple_of(c * rows, rows), rows)], hid.at[c, pl.ds(0, rows)], in_sem.at[c])

    def start_gu(layer, t):
        for u in range(2):
            gu_copy(layer, t, u).start()

    for t in range(t_qkv):
        for u in range(2):
            qkv_copy(0, t, u).start()
    prompt_copy(0).start()
    for t in range(t_out):
        out_copy(0, t).start()
    for c in range(1, CHUNKS):
        prompt_copy(c).start()

    def pair_copy(g):
        s = lax.rem(g, 2)
        return remote(part.at[lax.rem(g, 3), :, 1 - core], pair_in.at[s], pair_s.at[s], pair_r.at[s], to_pair)

    def half_pair_copy(g):
        s = lax.rem(g, 2)
        return remote(part.at[lax.rem(g, 3), grp, 1 - core], pair_in.at[s, grp], pair_s.at[s], pair_r.at[s], to_pair)

    def r1_copy(g, d):
        s = lax.rem(g, 2)
        return remote(part_block(g, c_far, d * sub, sub), ring1.at[s, d], r1_s.at[d], r1_r.at[s, d], (to_right, to_left)[d])

    def r2_copy(g, d):
        s = lax.rem(g, 2)
        return remote(part_block(g, (c_right, c_left)[d], 0, own), ring2.at[s, d], r2_s.at[d], r2_r.at[s, d], (to_right, to_left)[d])

    def r2_mate(g, d):
        s = lax.rem(g, 2)
        return remote(part_block(g, c_mate, 0, own), ring2.at[s, d], r2_s.at[d], r2_r.at[s, d], to_mate)

    def a1_copy(g, d):
        c = lax.rem(g, CHUNKS)
        ref = hid.at[c, pl.ds(block_row(chip, core), own)]
        return remote(ref, ref, a1_s.at[d], a1_r.at[c, d], (to_right, to_left)[d])

    def a1_mate(g, d):
        c = lax.rem(g, CHUNKS)
        ref = hid.at[c, pl.ds(block_row(chip, core), own)]
        return remote(ref, ref, a1_s.at[d], a1_r.at[c, d], to_mate)

    def a2_copy(g, d):
        c = lax.rem(g, CHUNKS)
        base = pl.multiple_of(block_row((c_left, c_right)[d], core) + d * sub, sub)
        ref = hid.at[c, pl.ds(base, sub)]
        return remote(ref, ref, a2_s.at[d], a2_r.at[c, d], (to_right, to_left)[d])

    def d_copy(g, i, of=None):
        c = lax.rem(g, CHUNKS)
        ref = hid.at[c, pl.ds(block_row((chip, c_left, c_right, c_far)[i] if of is None else of, core), own)]
        return remote(ref, ref, d_s.at[i], d_r.at[c, i], to_pair)

    def by_stage(g, stage, then, other):
        is_it = lax.div(g, CHUNKS) == stage

        @pl.when(is_it)
        def _():
            then()

        @pl.when(jnp.logical_not(is_it))
        def _():
            other()

    def when_chunk(g, body):
        @pl.when(jnp.logical_and(g >= 0, g < n_steps))
        def _():
            body(g)

    def add_pair(g, gi):
        slot = lax.rem(g, 3)
        s = lax.rem(g, 2)

        @pl.loop(0, seg // PAD)
        def _(i):
            loc = pl.ds(pl.multiple_of(i * PAD, PAD), PAD)
            part[slot, gi, core, loc] = (part[slot, gi, core, loc].astype(F32) + pair_in[s, gi, loc].astype(F32)).astype(BF16)

    def e0(g):
        by_stage(g, swap_stage, lambda: half_pair_copy(g).start(), lambda: pair_copy(g).start())

    def e1(g):
        def swapped():
            half_pair_copy(g).wait_recv()
            half_pair_copy(g).wait_send()
            add_pair(g, grp)

        def usual():
            pair_copy(g).wait_recv()
            pair_copy(g).wait_send()
            for gi in range(2):
                add_pair(g, gi)
            for d in range(2):
                r1_copy(g, d).start()

        by_stage(g, swap_stage, swapped, usual)

    def e2(g):
        def usual():
            s = lax.rem(g, 2)
            for d in range(2):
                r1_copy(g, d).wait_send()
                r1_copy(g, d).wait_recv()
            for d in range(2):
                ref = part_block(g, (c_right, c_left)[d], d * sub, sub)
                ref[...] = (ref[...].astype(F32) + ring1[s, d].astype(F32)).astype(BF16)
                r2_copy(g, d).start()

        by_stage(g, swap_stage, lambda: r2_mate(g, mate_out).start(), usual)

    def e3(g):
        s = lax.rem(g, 2)
        c = lax.rem(g, CHUNKS)
        st = lax.div(g, CHUNKS)
        mine = part_block(g, chip, 0, own)
        base = block_row(chip, core)

        def finish(totals):
            def new_rows(i):
                loc = pl.ds(i * PAD, PAD)
                dst = pl.ds(pl.multiple_of(base + i * PAD, PAD), PAD)
                total = mine[loc].astype(F32)
                for d in totals:
                    total = total + ring2[s, d, loc].astype(F32)
                return loc, dst, (resid[c, loc].astype(F32) + total.astype(BF16).astype(F32)).astype(BF16)

            @pl.when(st < n_stage - 1)
            def _():
                gain = gains[jnp.minimum(st + 1, n_stage - 1)]
                for i in range(own // PAD):
                    loc, dst, new = new_rows(i)
                    resid[c, loc] = new
                    hid[c, dst] = norm_rows(new.astype(F32), gain)

            @pl.when(st == n_stage - 1)
            def _():
                for i in range(own // PAD):
                    _, dst, new = new_rows(i)
                    hid[c, dst] = new

        def swapped():
            r2_mate(g, mate_out).wait_send()
            r2_mate(g, mate_in).wait_recv()
            finish((mate_in,))

        def usual():
            for d in range(2):
                r2_copy(g, d).wait_send()
                r2_copy(g, d).wait_recv()
            finish((0, 1))

        by_stage(g, swap_stage, swapped, usual)

        def to_both():
            for d in range(2):
                a1_copy(g, d).start()

        by_stage(g, swap_stage - 1, lambda: a1_mate(g, mate_out).start(), to_both)
        d_copy(g, 0).start()

    def e4(g):
        def swapped():
            a1_mate(g, mate_out).wait_send()
            a1_mate(g, mate_in).wait_recv()
            d_copy(g, 0).wait_send()
            d_copy(g, 1, c_mate).start()

        def usual():
            for d in range(2):
                a1_copy(g, d).wait_send()
                a1_copy(g, d).wait_recv()
                a2_copy(g, d).start()
            d_copy(g, 0).wait_send()
            d_copy(g, 1).start()
            d_copy(g, 2).start()

        by_stage(g, swap_stage - 1, swapped, usual)

    def e5(g):
        def usual():
            for d in range(2):
                a2_copy(g, d).wait_send()
                a2_copy(g, d).wait_recv()
            d_copy(g, 1).wait_send()
            d_copy(g, 2).wait_send()
            d_copy(g, 3).start()

        by_stage(g, swap_stage - 1, lambda: d_copy(g, 1, c_mate).wait_send(), usual)

    def e6(g):
        def swapped():
            for i in range(2):
                d_copy(g, i).wait_recv()

        def usual():
            d_copy(g, 3).wait_send()
            for i in range(4):
                d_copy(g, i).wait_recv()

        by_stage(g, swap_stage - 1, swapped, usual)

    def y_pair_copy(st):
        return remote(y_part.at[st], y_pair.at[st], yp_s.at[st], yp_r.at[st], to_pair)

    def y_chip_copy(st, i):
        return remote(y_chip.at[st, chip], y_chip.at[st, chip], yc_s.at[i], yc_r.at[st, i], (to_right, to_left, to_far)[i])

    first_copy = remote(tail_out.at[:, pl.ds(0, d_model)], y_row, edge_s.at[0], edge_r.at[0], to_down)
    tail_copy = remote(tail_out, tail_in, edge_s.at[1], edge_r.at[1], to_up)

    def put_y(gain, at):
        row = norm_rows(y_row[...], gain)
        hid[CHUNKS - 1, pl.ds(at, PAD)] = jnp.broadcast_to(row.astype(F32), (PAD, d_model)).astype(BF16)

    def y_sum(st):
        y_pair_copy(st).wait_send()
        y_pair_copy(st).wait_recv()
        y_chip[st, chip] = y_part[st] + y_pair[st]
        for i in range(3):
            y_chip_copy(st, i).start()

    def y_done(st):
        for i in range(3):
            y_chip_copy(st, i).wait_send()
            y_chip_copy(st, i).wait_recv()
        total = y_chip[st, 0]
        for i in range(1, n_chip):
            total = total + y_chip[st, i]
        y_row[...] = y_row[...] + total.astype(BF16).astype(F32)

        @pl.when(st < n_stage - 1)
        def _():
            at = jnp.where(st + 1 == swap_stage, grp * half + half, rows)
            put_y(gains[jnp.minimum(st + 1, n_stage - 1)], pl.multiple_of(at, PAD))

        @pl.when(st == n_stage - 1)
        def _():
            tail_out[:, pl.ds(0, d_model)] = y_row[...]
            tail_copy.start()

    def c0_copy(layer):
        src = kv0 if layer == 0 else kv1.at[0]
        return remote(src, cb0.at[layer], c0_s.at[layer], c0_r.at[layer], to_up)

    def c1_copy(layer, i):
        def tokens(c):
            return pl.ds(pl.multiple_of(c * tok_chip, tok_chip), tok_chip)

        src, dst, to = (
            (cb0.at[layer, :, tokens(c_right)], cb1.at[layer, 0], to_right),
            (cb0.at[layer, :, tokens(c_left)], cb1.at[layer, 1], to_left),
            (cb0.at[layer, 0, tokens(c_far)], relay.at[layer, 0], to_right),
            (cb0.at[layer, 1, tokens(c_far)], relay.at[layer, 1], to_left),
            (relay.at[layer, 0], cb1.at[layer, 2, 0], to_right),
            (relay.at[layer, 1], cb1.at[layer, 2, 1], to_left),
        )[i]
        return remote(src, dst, c1_s.at[layer, i], c1_r.at[layer, i], to)

    def c2_source(layer, i, n, which):
        off = pl.multiple_of(which * tok_dev, tok_dev)
        if i < 3:
            return cb1.at[layer, i, n, pl.ds(off, tok_dev)], (c_left, c_right, c_far)[i]
        return cb0.at[layer, n, pl.ds(pl.multiple_of(chip * tok_chip + off, tok_dev), tok_dev)], chip

    def c2_copy(layer, i, n):
        src, src_chip = c2_source(layer, i, n, 1 - core)
        return remote(src, (k_tok, v_tok)[n].at[layer, 2 * src_chip + core], c2_s.at[layer, i, n], c2_r.at[layer, i, n], to_pair)

    def c2_local(layer, i, n):
        src, src_chip = c2_source(layer, i, n, core)
        return pltpu.make_async_copy(src, (k_tok, v_tok)[n].at[layer, 2 * src_chip + core], c2_l.at[layer, i, n])

    def cache_events(g):
        for layer in range(n_layers):
            at = CACHE_STEPS[layer]

            @pl.when(g == at[0])
            def _():
                c0_copy(layer).start()

            @pl.when(g == at[1])
            def _():
                c0_copy(layer).wait_send()
                c0_copy(layer).wait_recv()
                c1_copy(layer, 0).start()
                c1_copy(layer, 1).start()

            @pl.when(g == at[2])
            def _():
                c1_copy(layer, 2).start()
                c1_copy(layer, 3).start()

            @pl.when(g == at[3])
            def _():
                for i in (2, 3):
                    c1_copy(layer, i).wait_send()
                    c1_copy(layer, i).wait_recv()
                for i in (4, 5):
                    c1_copy(layer, i).start()

            @pl.when(g == at[4])
            def _():
                for i in (0, 1, 4, 5):
                    c1_copy(layer, i).wait_send()
                    c1_copy(layer, i).wait_recv()
                for i in range(4):
                    for n in range(2):
                        c2_copy(layer, i, n).start()
                        c2_local(layer, i, n).start()

            @pl.when(g == at[5])
            def _():
                for i in range(4):
                    for n in range(2):
                        c2_copy(layer, i, n).wait_send()
                        c2_copy(layer, i, n).wait_recv()
                        c2_local(layer, i, n).wait()

    n_wq = n_slots
    n_wx = len(WX_STEPS)
    o_piece = o_rows // n_ho // (n_wx - n_wq)

    def wx_ref(i, quarter, first=0, parts=1, given=False):
        size = (d_model // n_ho if i < n_wq else o_piece) // parts
        if i < n_wq:
            base = quarter * (d_model // n_ho)
            ref = w_qkv.at[swap_layer, i] if given else wq_x.at[i]
        else:
            base = quarter * (o_rows // n_ho) + (i - n_wq) * o_piece
            ref = w_o.at[swap_layer] if given else wo_x
        return ref.at[pl.ds(pl.multiple_of(base + first * size, size), size)]

    def wx_copy(i):
        return remote(wx_ref(i, ho, given=True), wx_ref(i, ho), wx_s.at[i], wx_r.at[i], to_swap)

    def wy_copy(i, j):
        ref = (
            wx_ref(i, ho),
            wx_ref(i, ho),
            wx_ref(i, lax.rem(ho + n_ho - 1, n_ho), 0, 2),
            wx_ref(i, lax.rem(ho + 1, n_ho), 1, 2),
        )[j]
        return remote(ref, ref, wy_s.at[i, j], wy_r.at[i, j], (to_up, to_down)[j % 2])

    def swap_events(g):
        for i in range(n_wx):
            @pl.when(g == WX_STEPS[i])
            def _():
                wx_copy(i).start()

    def share_events(g):
        for i in range(n_wx):
            share = WX_STEPS[i] + 2 + (i == n_wx - 2)

            @pl.when(g == share)
            def _():
                wx_copy(i).wait_send()
                wx_copy(i).wait_recv()
                for j in (0, 1):
                    wy_copy(i, j).start()

            @pl.when(g == share + 1)
            def _():
                for j in (0, 1):
                    wy_copy(i, j).wait_send()
                    wy_copy(i, j).wait_recv()
                for j in (2, 3):
                    wy_copy(i, j).start()

    def swap_arrived(pieces):
        for i in pieces:
            for j in (2, 3):
                wy_copy(i, j).wait_send()
                wy_copy(i, j).wait_recv()

    def store_part(g, t, acc):
        cols = pl.ds(pl.multiple_of(t * COLS_B, COLS_B), COLS_B)
        part[lax.rem(g, 3), :, :, :, cols] = acc[:rows].astype(BF16).reshape(2, 2, seg, COLS_B)
        y_part[lax.div(g, CHUNKS), :, cols] = acc[rows:rows + 1]

    def first_norm(c):
        prompt_copy(c).wait()
        gain = gains[0]
        for i in range(own // PAD):
            resid[c, pl.ds(i * PAD, PAD)] = hid[c, pl.ds(pl.multiple_of(block_row(chip, core) + i * PAD, PAD), PAD)]

        @pl.loop(0, rows // NORM_ROWS)
        def _(i):
            loc = pl.ds(pl.multiple_of(i * NORM_ROWS, NORM_ROWS), NORM_ROWS)
            hid[c, loc] = norm_rows(hid[c, loc].astype(F32), gain)

        @pl.when(c == CHUNKS - 1)
        def _():
            first_copy.wait_send()
            first_copy.wait_recv()
            put_y(gain, rows)

    def attention(c, keys, n_rows, row_of, before_diag, put):
        units = range(len(keys))

        def loc_of(j):
            return pl.ds(pl.multiple_of(j * rows, rows), rows)

        def score(u, loc):
            return lax.dot_general(qry[pl.ds(u * n_rows, n_rows)], keys[u][0, loc], CONTRACT_LAST, preferred_element_type=F32) * scale

        def fold(op, x, s):
            for b in range(rows // head):
                x = op(x, s[:, b * head:(b + 1) * head])
            return x

        def first(j, tops):
            loc = loc_of(j)
            new = []
            for u in units:
                s = score(u, loc)
                scores[pl.ds(u * n_rows, n_rows), loc] = s
                new.append(fold(jnp.maximum, tops[u], s))
            return tuple(new)

        lowest = jnp.full((n_rows, head), -jnp.inf, F32)
        tops = lax.fori_loop(0, c, first, tuple(lowest for _ in units))
        before_diag()
        diag = loc_of(c)
        causal = row_of(lax.broadcasted_iota(jnp.int32, (n_rows, rows), 0)) >= lax.broadcasted_iota(jnp.int32, (n_rows, rows), 1)
        row_top = []
        for u in units:
            s = jnp.where(causal, score(u, diag), -jnp.inf)
            scores[pl.ds(u * n_rows, n_rows), diag] = s
            row_top.append(jnp.max(fold(jnp.maximum, tops[u], s), axis=1, keepdims=True))

        def second(j, carry):
            loc = loc_of(j)
            new = []
            for u in units:
                denom, numer = carry[u]
                p = jnp.exp(scores[pl.ds(u * n_rows, n_rows), loc] - row_top[u])
                new.append((fold(jnp.add, denom, p), numer + jnp.dot(p.astype(BF16), keys[u][1, loc], preferred_element_type=F32)))
            return tuple(new)

        zero = jnp.zeros((n_rows, head), F32)
        sums = lax.fori_loop(0, c + 1, second, tuple((zero, zero) for _ in units))
        for u in units:
            denom, numer = sums[u]
            put(u, (numer / jnp.sum(denom, axis=1, keepdims=True)).astype(BF16))

    def attention_new(keys, att, at):
        q = qry_new[...].reshape(n_group * PAD, head)
        k_row = k_new[...].astype(F32)[:1]
        v_row = v_new[...].astype(F32)[:1]
        s_new = jnp.sum(q.astype(F32) * k_row, axis=1, keepdims=True) * scale
        s_old = lax.dot_general(q, keys[0], CONTRACT_LAST, preferred_element_type=F32) * scale
        top = jnp.maximum(jnp.max(s_old, axis=1, keepdims=True), s_new)
        p_old = jnp.exp(s_old - top)
        p_new = jnp.exp(s_new - top)
        denom = jnp.sum(p_old, axis=1, keepdims=True) + p_new
        numer = jnp.dot(p_old.astype(BF16), keys[1], preferred_element_type=F32) + p_new * v_row
        out = (numer / denom).astype(BF16)
        for h in range(n_group):
            att[pl.ds(at, PAD), pl.ds(h * head, head)] = out[h * PAD:(h + 1) * PAD]

    def put_new_kv(layer):
        tail_out[:, pl.ds(d_model + 2 * layer * head, head)] = k_new[...].astype(F32)[:1]
        tail_out[:, pl.ds(d_model + (2 * layer + 1) * head, head)] = v_new[...].astype(F32)[:1]

    def next_is_mlp(layer, c):
        @pl.when(c == CHUNKS - 1)
        def _():
            for t in range(2):
                start_gu(layer, t)

    def step_a(g, c):
        layer = 0
        first_norm(c)

        @pl.when(c == 0)
        def _():
            for t in range(t_qkv):
                for u in range(2):
                    qkv_copy(layer, t, u).wait()

        for t in range(t_qkv):
            out = jnp.dot(hid[c], wa[t], preferred_element_type=F32).astype(BF16)
            if t < t_qkv - 1:
                for u in range(2):
                    h = 2 * t + u
                    qry[pl.ds(h * rows, rows)] = out[:rows, u * head:(u + 1) * head]
                    qry_new[h] = out[rows:, u * head:(u + 1) * head]
            else:
                loc = pl.ds(pl.multiple_of(c * rows, rows), rows)
                kv0[0, loc] = out[:rows, :head]
                kv0[1, loc] = out[:rows, head:]
                k_new[...] = out[rows:, :head]
                v_new[...] = out[rows:, head:]

        next_is_mlp(layer, c)
        when_chunk(g - 1, e1)

        def put(u, o):
            att0[pl.ds(0, rows), pl.ds(u * head, head)] = o

        attention(c, [kv0] * n_group, rows, lambda r: r, lambda: None, put)

        @pl.when(c == CHUNKS - 1)
        def _():
            attention_new(kv0, att0, rows)
            put_new_kv(layer)

        @pl.when(c == 0)
        def _():
            for t in range(t_out):
                out_copy(layer, t).wait()

        for t in range(t_out):
            store_part(g, t, jnp.dot(att0[...], out_tile(t)[...], preferred_element_type=F32))

        @pl.when(c == CHUNKS - 1)
        def _():
            for t in range(SLOTS_B):
                down_copy(layer, 0, t).start()

    def kx_copy(c, o):
        loc = pl.ds(pl.multiple_of(c * rows + grp * half, half), half)
        return remote(kv1.at[o, :, loc], kv1.at[1 - o, :, loc], kx_s.at[o], kx_r.at[c, 1 - o], to_swap)

    def swap_qkv(c):
        lhs = pl.ds(pl.multiple_of(grp * half, half), half + PAD)
        loc = pl.ds(pl.multiple_of(c * rows + grp * half, half), half)
        for pair in range(t_qkv):
            slot = lax.rem(c * t_qkv + pair, 2) * 2
            for v in range(2):
                t = 2 * pair + v
                for u in range(2):
                    swap_qkv_copy(slot + v, t, u).wait()
                out = jnp.dot(hid[c, lhs], wa[slot + v], preferred_element_type=F32).astype(BF16)
                o, r = t // t_qkv, t % t_qkv
                if r < t_qkv - 1:
                    for u in range(2):
                        h = 2 * r + u
                        qry[pl.ds((o * n_group + h) * half, half)] = out[:half, u * head:(u + 1) * head]
                        if o == 0:
                            qry_new[h] = out[half:, u * head:(u + 1) * head]
                else:
                    kv1[o, 0, loc] = out[:half, :head]
                    kv1[o, 1, loc] = out[:half, head:]
                    if o == 0:
                        k_new[...] = out[half:, :head]
                        v_new[...] = out[half:, head:]

            if pair + 2 < t_qkv:
                start_swap_qkv(c, pair + 2)
            else:
                @pl.when(c + 1 < CHUNKS)
                def _():
                    start_swap_qkv(c + 1, pair + 2 - t_qkv)

        for o in range(2):
            kx_copy(c, o).start()

    def step_s(g, c):
        def before_diag():
            for o in range(2):
                kx_copy(c, o).wait_send()
                kx_copy(c, 1 - o).wait_recv()

        def put(u, out):
            for h in range(n_group):
                att1[pl.ds(0, half), pl.ds((u * n_group + h) * head, head)] = out[h * half:(h + 1) * half]

        attention(c, [kv1.at[0], kv1.at[1]], n_group * half, lambda r: lax.rem(r, half) + grp * half, before_diag, put)

        @pl.when(c == CHUNKS - 1)
        def _():
            attention_new(kv1.at[0], att1, half)
            put_new_kv(swap_layer)

        when_chunk(g - 1, e1)

    def swap_out(g, c):
        @pl.when(c == 0)
        def _():
            swap_arrived(range(n_wq, n_wx))
            for t in range(SLOTS_B):
                for v in range(2):
                    swap_out_copy(0, t, v).start()

        for t in range(t_out):
            slot = lax.rem(c * t_out + t, SLOTS_B)
            for v in range(2):
                swap_out_copy(c, t, v).wait()
            cols = pl.ds(t * COLS_B, COLS_B)
            acc = jnp.dot(att1[...], wb[slot, pl.ds(0, 2 * o_rows)], preferred_element_type=F32)
            part[lax.rem(g, 3), grp, :, :, cols] = acc[:half].astype(BF16).reshape(2, seg, COLS_B)
            y_part[swap_stage, :, cols] = acc[half:half + 1]
            ahead = t + SLOTS_B
            if ahead < t_out:
                for v in range(2):
                    swap_out_copy(c, ahead, v).start()
            else:
                @pl.when(c + 1 < CHUNKS)
                def _():
                    for v in range(2):
                        swap_out_copy(c + 1, ahead - t_out, v).start()

        @pl.when(c == CHUNKS - 1)
        def _():
            for t in range(SLOTS_B):
                down_copy(swap_layer, 0, t).start()

    def step_m(g, layer, c):
        more = layer < swap_layer

        @pl.loop(0, t_gu)
        def _(t):
            for u in range(2):
                gu_copy(layer, t, u).wait()
            slot = lax.rem(t, 2) * 2
            gate = jnp.dot(hid[c], wa[slot], preferred_element_type=F32)
            up = jnp.dot(hid[c], wa[slot + 1], preferred_element_type=F32)
            act[:, pl.ds(pl.multiple_of(t * COLS_A, COLS_A), COLS_A)] = (jax.nn.silu(gate) * up).astype(BF16)

            @pl.when(jnp.logical_or(t + 2 < t_gu, c + 1 < CHUNKS))
            def _():
                start_gu(layer, lax.rem(t + 2, t_gu))

        @pl.when(jnp.logical_and(c == CHUNKS - 1, more))
        def _():
            swap_arrived(range(n_wq))
            start_swap_qkv(0, 0)

        when_chunk(g - 1, e1)

        @pl.loop(0, t_out)
        def _(t):
            down_copy(layer, c, t).wait()
            store_part(g, t, jnp.dot(act[...], wb[lax.rem(c * t_out + t, SLOTS_B)], preferred_element_type=F32))
            ahead = t + SLOTS_B

            @pl.when(jnp.logical_or(ahead < t_out, c + 1 < CHUNKS))
            def _():
                down_copy(layer, c + lax.div(ahead, t_out), lax.rem(ahead, t_out)).start()

        @pl.when(jnp.logical_and(c == CHUNKS - 1, more))
        def _():
            start_swap_qkv(0, 1)

    for layer in range(n_layers):
        gains[2 * layer] = g_attn[layer:layer + 1]
        gains[2 * layer + 1] = g_mlp[layer:layer + 1]
    for c in range(CHUNKS):
        hid[c, pl.ds(rows, PAD)] = jnp.zeros((PAD, d_model), BF16)
    att0[pl.ds(rows, PAD)] = jnp.zeros((PAD, o_rows), BF16)
    att1[pl.ds(half, PAD)] = jnp.zeros((PAD, 2 * o_rows), BF16)
    pl.semaphore_wait(barrier, len(peers))
    first_copy.start()

    @pl.loop(0, n_steps + LAGS)
    def _(g):
        st = lax.div(g, CHUNKS)
        c = lax.rem(g, CHUNKS)
        layer = lax.div(st, 2)
        when_chunk(g - 6, e6)
        when_chunk(g - 5, e5)
        when_chunk(g - 4, e4)
        when_chunk(g - 3, e3)
        when_chunk(g - 2, e2)

        @pl.when(jnp.logical_and(c == 1, jnp.logical_and(st >= 1, st <= n_stage)))
        def _():
            y_sum(st - 1)

        @pl.when(jnp.logical_and(c == 2, jnp.logical_and(st >= 1, st <= n_stage)))
        def _():
            y_done(st - 1)

        share_events(g)

        @pl.when(g == 0)
        def _():
            swap_events(g)

        @pl.when(st == 0)
        def _():
            step_a(g, c)

        @pl.when(st == swap_stage)
        def _():
            step_s(g, c)

        @pl.when(jnp.logical_and(g < n_steps, lax.rem(st, 2) == 1))
        def _():
            step_m(g, layer, c)

        first_swap = swap_stage * CHUNKS - 1

        @pl.when(jnp.logical_and(g >= first_swap, g < first_swap + CHUNKS))
        def _():
            swap_qkv(g - first_swap)

        @pl.when(st == swap_stage)
        def _():
            swap_out(g, c)

        @pl.when(g == first_swap + CHUNKS - 1)
        def _():
            next_is_mlp(swap_layer, CHUNKS - 1)

        @pl.when(g > 0)
        def _():
            swap_events(g)

        cache_events(g)

        @pl.when(g == n_steps)
        def _():
            e1(g - 1)

        @pl.when(g < n_steps)
        def _():
            e0(g)

        @pl.when(jnp.logical_and(g < n_steps, c == CHUNKS - 1))
        def _():
            y_pair_copy(st).start()

    tail_copy.wait_send()
    tail_copy.wait_recv()
    tail[...] = tail_in[...]


def finish_kernel(hid, tail, k_tok, v_tok, x_last, k_cache, v_cache, y_last, kv_new, by_head, by_token, x_sem, in_sem, out_sem):
    n_layers = k_tok.shape[0]
    rows = x_last.shape[0] // CHUNKS
    d_model = y_last.shape[1]
    head = k_tok.shape[3]

    def x_copy(c):
        return pltpu.make_async_copy(hid.at[c, pl.ds(0, rows)], x_last.at[pl.ds(c * rows, rows)], x_sem.at[c])

    def in_copy(n):
        return pltpu.make_async_copy((k_tok, v_tok)[n], by_head.at[n], in_sem.at[n])

    def out_copy(n):
        return pltpu.make_async_copy(by_token.at[n], (k_cache, v_cache)[n], out_sem.at[n])

    for n in range(2):
        in_copy(n).start()
    for c in range(CHUNKS):
        x_copy(c).start()
    y_last[...] = tail[:, :d_model]
    kv_new[...] = jnp.concatenate([tail[:, d_model + i * head:d_model + (i + 1) * head] for i in range(2 * n_layers)], axis=0).astype(BF16)
    for n in range(2):
        in_copy(n).wait()
        for layer in range(n_layers):
            by_token[n, layer] = jnp.transpose(by_head[n, layer], (1, 0, 2))
        out_copy(n).start()
    for n in range(2):
        out_copy(n).wait()
    for c in range(CHUNKS):
        x_copy(c).wait()


def solution(mesh):
    n_ho, n_tp = mesh.shape['ho'], mesh.shape['tp']
    row_axes = ('pairs', 'ho')
    in_specs = (P('pairs'), P(row_axes), P(None, None, 'tp'), P(None, 'tp'), P(None, None, 'tp'), P(None, None, 'tp'), P(None, 'tp'), P(), P())
    out_specs = (P(row_axes), P(row_axes), P(row_axes, None, 'tp'), P(row_axes, None, 'tp'), P(row_axes, None, None, 'tp'))

    def device_program(prompts, y_first, w_qkv, w_o, w_gate, w_up, w_down, g_attn, g_mlp):
        n_layers, d_model, _, n_slots, head = w_qkv.shape
        n_tok = prompts.shape[1]
        ff = w_gate.shape[2]
        rows = n_tok // CHUNKS
        half = rows // 2
        seg = half // 2
        own = half // (n_tp // 2)
        n_stage = 2 * n_layers
        group = n_slots - 2
        o_rows = group * head
        tok_dev = n_tok // n_tp
        n_wx = len(WX_STEPS)
        wq = jnp.transpose(w_qkv[:, :, 0], (0, 2, 1, 3))
        tail_len = d_model + 2 * n_layers * head
        any_spec = pl.BlockSpec(memory_space=pl.ANY)
        vmem_spec = pl.BlockSpec(memory_space=pltpu.VMEM)
        hbm_spec = pl.BlockSpec(memory_space=pltpu.HBM)
        dma = pltpu.SemaphoreType.DMA
        both, both_ways, by_chunk, by_chunk_two = dma((2,)), dma((2, 2)), dma((CHUNKS,)), dma((CHUNKS, 2))
        by_stage, by_layer, cache = dma((n_stage,)), dma((n_layers,)), dma((n_layers, 4, 2))
        vmem = pltpu.VMEM
        hid, tail, k_tok, v_tok, *_ = pl.pallas_call(
            functools.partial(group_kernel, n_ho, n_tp),
            out_shape=(
                vmem((CHUNKS, rows + PAD, d_model), BF16),
                jax.ShapeDtypeStruct((1, tail_len), F32),
                jax.ShapeDtypeStruct((n_layers, n_tp, tok_dev, head), BF16),
                jax.ShapeDtypeStruct((n_layers, n_tp, tok_dev, head), BF16),
                jax.ShapeDtypeStruct((n_slots, d_model, head), BF16),
                jax.ShapeDtypeStruct((o_rows, d_model), BF16),
                jax.ShapeDtypeStruct((n_layers, 2, n_tok, head), BF16),
                jax.ShapeDtypeStruct((n_layers, 3, 2, 2 * tok_dev, head), BF16),
                jax.ShapeDtypeStruct((n_layers, 2, 2 * tok_dev, head), BF16),
            ),
            in_specs=[any_spec, vmem_spec, any_spec, any_spec, any_spec, any_spec, any_spec, vmem_spec, vmem_spec],
            out_specs=(vmem_spec, vmem_spec) + (any_spec,) * 7,
            scratch_shapes=[
                vmem((3, 2, 2, seg, d_model), BF16),
                vmem((2, 2, seg, d_model), BF16),
                vmem((2, 2, own // 2, d_model), BF16),
                vmem((2, 2, own, d_model), BF16),
                vmem((CHUNKS, own, d_model), BF16),
                vmem((2, n_tok, head), BF16),
                vmem((2, 2, n_tok, head), BF16),
                vmem((group * rows, n_tok), F32),
                vmem((group * rows, head), BF16),
                vmem((group, PAD, head), BF16),
                vmem((rows + PAD, o_rows), BF16),
                vmem((half + PAD, 2 * o_rows), BF16),
                vmem((rows + PAD, ff), BF16),
                vmem((4, d_model, COLS_A), BF16),
                vmem((SLOTS_B, ff, COLS_B), BF16),
                vmem((PAD, head), BF16),
                vmem((PAD, head), BF16),
                vmem((n_stage, 1, d_model), F32),
                vmem((1, d_model), F32),
                vmem((n_stage, 1, d_model), F32),
                vmem((n_stage, 1, d_model), F32),
                vmem((n_stage, n_tp // 2, 1, d_model), F32),
                vmem((1, tail_len), F32),
                vmem((1, tail_len), F32),
                dma((4, 2)), dma((2 * SLOTS_B,)), by_chunk,
                both, both, both, both_ways, both, both_ways,
                both, by_chunk_two, both, by_chunk_two, dma((4,)), dma((CHUNKS, 4)),
                by_stage, by_stage, dma((3,)), dma((n_stage, 3)), both, both,
                by_layer, by_layer, dma((n_layers, 6)), dma((n_layers, 6)),
                cache, cache, cache,
                both, by_chunk_two, dma((n_wx,)), dma((n_wx,)), dma((n_wx, 4)), dma((n_wx, 4)),
            ],
            compiler_params=pltpu.CompilerParams(collective_id=0, has_side_effects=True, vmem_limit_bytes=VMEM_LIMIT),
            name="group_step",
        )(prompts, y_first, wq, w_o, w_gate, w_up, w_down, g_attn, g_mlp)
        x_last, k_cache, v_cache, y_last, kv_new = pl.pallas_call(
            finish_kernel,
            out_shape=(
                jax.ShapeDtypeStruct((n_tok, d_model), BF16),
                jax.ShapeDtypeStruct((n_layers, tok_dev, n_tp, head), BF16),
                jax.ShapeDtypeStruct((n_layers, tok_dev, n_tp, head), BF16),
                jax.ShapeDtypeStruct((1, d_model), F32),
                jax.ShapeDtypeStruct((2 * n_layers, head), BF16),
            ),
            in_specs=[any_spec, vmem_spec, hbm_spec, hbm_spec],
            out_specs=(any_spec, any_spec, any_spec, vmem_spec, vmem_spec),
            scratch_shapes=[
                vmem((2, n_layers, n_tp, tok_dev, head), BF16),
                vmem((2, n_layers, tok_dev, n_tp, head), BF16),
                by_chunk, both, both,
            ],
            compiler_params=pltpu.CompilerParams(vmem_limit_bytes=16 << 20),
            name="finish",
        )(hid, tail, k_tok, v_tok)
        kv_new = kv_new.reshape(n_layers, 2, 1, head)
        return x_last[None], y_last, k_cache[None], v_cache[None], kv_new[None]

    return jax.shard_map(device_program, mesh=mesh, in_specs=in_specs, out_specs=out_specs, check_vma=False)
```

```python
import functools

import jax
import jax.numpy as jnp
from jax import lax
from jax.experimental import pallas as pl
from jax.experimental.pallas import tpu as pltpu
from jax.sharding import PartitionSpec as P

NORM_EPS = 1e-5
MESH = pl.DeviceIdType.MESH
CHUNKS = 8
PAD = 16
COLS_A = 256
COLS_B = 1024
LAGS = 6
NORM_ROWS = 32
VMEM_LIMIT = 46 << 20
WX_STEPS = (0, 0, 1, 2, 10, 11, 11, 12, 12, 13)
CACHE_STEPS = ((8, 16, 18, 20, 22, 24), (24, 26, 27, 29, 31, 33))
SLOTS_B = 3
CONTRACT_LAST = (((1,), (1,)), ((), ()))
F32 = jnp.float32
BF16 = jnp.bfloat16


def norm_rows(rows_f32, gain):
    inv_rms = lax.rsqrt(jnp.mean(rows_f32 * rows_f32, axis=-1, keepdims=True) + NORM_EPS)
    return (rows_f32 * inv_rms * gain).astype(BF16)


def remote(src, dst, send, recv, device):
    return pltpu.make_async_remote_copy(src_ref=src, dst_ref=dst, send_sem=send, recv_sem=recv, device_id=device, device_id_type=MESH)


def chip_group(chip):
    return lax.rem(lax.div(chip + 1, 2) + 1, 2)


def chip_member(chip):
    return lax.div(chip, 2)


def group_kernel(n_ho, n_tp, prompts, y_first, w_qkv, w_o, w_gate, w_up, w_down, g_attn, g_mlp, hid, tail, k_tok, v_tok, wq_x, wo_x, cb0, cb1, relay,
                 part, pair_in, ring1, ring2, resid, kv0, kv1, scores, qry, qry_new, att0, att1, act, wa, wb,
                 k_new, v_new, gains, y_row, y_part, y_pair, y_chip, tail_out, tail_in,
                 wa_sem, wb_sem, in_sem, pair_s, pair_r, r1_s, r1_r, r2_s, r2_r, a1_s, a1_r, a2_s, a2_r, d_s, d_r,
                 yp_s, yp_r, yc_s, yc_r, edge_s, edge_r, c0_s, c0_r, c1_s, c1_r, c2_s, c2_r, c2_l, kx_s, kx_r, wx_s, wx_r, wy_s, wy_r):
    tp = lax.axis_index("tp")
    ho = lax.axis_index("ho")
    n_chip = n_tp // 2
    core = lax.rem(tp, 2)
    chip = lax.div(tp, 2)
    odd = lax.rem(chip, 2)
    to_right = {"tp": lax.rem(tp + 2, n_tp)}
    to_left = {"tp": lax.rem(tp + n_tp - 2, n_tp)}
    to_far = {"tp": lax.rem(tp + 4, n_tp)}
    to_pair = {"tp": tp + 1 - 2 * core}
    to_up = {"ho": lax.rem(ho + 1, n_ho)}
    to_down = {"ho": lax.rem(ho + n_ho - 1, n_ho)}
    c_right = lax.rem(chip + 1, n_chip)
    c_left = lax.rem(chip + n_chip - 1, n_chip)
    c_far = lax.rem(chip + 2, n_chip)
    c_mate = lax.rem(chip + n_chip + 2 * odd - 1, n_chip)
    to_mate = {"tp": lax.rem(tp + n_tp + 4 * odd - 2, n_tp)}
    to_swap = {"tp": lax.rem(tp + n_tp + 2 - 4 * odd, n_tp)}
    mate_out = 1 - odd
    mate_in = odd
    grp = chip_group(chip)

    n_layers, n_slots, d_model, head = w_qkv.shape
    n_group = n_slots - 2
    ff = w_gate.shape[2]
    n_tok = prompts.shape[1]
    rows = n_tok // CHUNKS
    half = rows // 2
    seg = half // 2
    own = half // n_chip
    sub = own // 2
    n_stage = 2 * n_layers
    n_steps = n_stage * CHUNKS
    swap_stage = n_stage - 2
    swap_layer = n_layers - 1
    o_rows = n_group * head
    o_per_slot = ff // o_rows
    t_qkv = n_slots * head // COLS_A
    t_gu = ff // COLS_A
    t_out = d_model // COLS_B
    tok_dev = n_tok // n_tp
    tok_chip = 2 * tok_dev
    scale = head ** -0.5

    def block_row(c, k):
        return pl.multiple_of(chip_group(c) * half + k * seg + chip_member(c) * own, own)

    def part_block(g, c, first, size):
        return part.at[lax.rem(g, 3), chip_group(c), core, pl.ds(pl.multiple_of(chip_member(c) * own + first, size), size)]

    tail_out[:, pl.ds(0, d_model)] = y_first[...].astype(F32)
    barrier = pltpu.get_barrier_semaphore()
    peers = (to_right, to_left, to_far, to_pair, to_up, to_down)
    for peer in peers:
        pl.semaphore_signal(barrier, inc=1, device_id=peer, device_id_type=MESH)

    def qkv_copy(layer, t, u):
        return pltpu.make_async_copy(w_qkv.at[layer, t * 2 + u], wa.at[t, :, pl.ds(u * head, head)], wa_sem.at[t, u])

    def swap_qkv_copy(slot, t, u):
        src = w_qkv.at[swap_layer, t * 2 + u] if t < t_qkv else wq_x.at[(t - t_qkv) * 2 + u]
        return pltpu.make_async_copy(src, wa.at[slot, :, pl.ds(u * head, head)], wa_sem.at[slot, u])

    def start_swap_qkv(c, pair):
        slot = lax.rem(c * t_qkv + pair, 2) * 2
        for v in range(2):
            for u in range(2):
                swap_qkv_copy(slot + v, 2 * pair + v, u).start()

    def gu_copy(layer, t, u):
        slot = lax.rem(t, 2) * 2 + u
        cols = pl.ds(pl.multiple_of(t * COLS_A, COLS_A), COLS_A)
        return pltpu.make_async_copy((w_gate, w_up)[u].at[layer, :, cols], wa.at[slot], wa_sem.at[slot, 0])

    def out_tile(t):
        return wb.at[t // o_per_slot, pl.ds((t % o_per_slot) * o_rows, o_rows)]

    def out_copy(layer, t):
        return pltpu.make_async_copy(w_o.at[layer, :, pl.ds(t * COLS_B, COLS_B)], out_tile(t), wb_sem.at[t])

    def swap_out_copy(c, t, v):
        slot = lax.rem(c * t_out + t, SLOTS_B)
        src = (w_o.at[swap_layer], wo_x)[v].at[:, pl.ds(t * COLS_B, COLS_B)]
        return pltpu.make_async_copy(src, wb.at[slot, pl.ds(v * o_rows, o_rows)], wb_sem.at[slot * 2 + v])

    def down_copy(layer, c, t):
        slot = lax.rem(c * t_out + t, SLOTS_B)
        cols = pl.ds(pl.multiple_of(t * COLS_B, COLS_B), COLS_B)
        return pltpu.make_async_copy(w_down.at[layer, :, cols], wb.at[slot], wb_sem.at[slot])

    def prompt_copy(c):
        return pltpu.make_async_copy(prompts.at[ho, pl.ds(pl.multiple_of(c * rows, rows), rows)], hid.at[c, pl.ds(0, rows)], in_sem.at[c])

    def start_gu(layer, t):
        for u in range(2):
            gu_copy(layer, t, u).start()

    for t in range(t_qkv):
        for u in range(2):
            qkv_copy(0, t, u).start()
    prompt_copy(0).start()
    for t in range(t_out):
        out_copy(0, t).start()
    for c in range(1, CHUNKS):
        prompt_copy(c).start()

    def pair_copy(g):
        s = lax.rem(g, 2)
        return remote(part.at[lax.rem(g, 3), :, 1 - core], pair_in.at[s], pair_s.at[s], pair_r.at[s], to_pair)

    def half_pair_copy(g):
        s = lax.rem(g, 2)
        return remote(part.at[lax.rem(g, 3), grp, 1 - core], pair_in.at[s, grp], pair_s.at[s], pair_r.at[s], to_pair)

    def r1_copy(g, d):
        s = lax.rem(g, 2)
        return remote(part_block(g, c_far, d * sub, sub), ring1.at[s, d], r1_s.at[d], r1_r.at[s, d], (to_right, to_left)[d])

    def r2_copy(g, d):
        s = lax.rem(g, 2)
        return remote(part_block(g, (c_right, c_left)[d], 0, own), ring2.at[s, d], r2_s.at[d], r2_r.at[s, d], (to_right, to_left)[d])

    def r2_mate(g, d):
        s = lax.rem(g, 2)
        return remote(part_block(g, c_mate, 0, own), ring2.at[s, d], r2_s.at[d], r2_r.at[s, d], to_mate)

    def a1_copy(g, d):
        c = lax.rem(g, CHUNKS)
        ref = hid.at[c, pl.ds(block_row(chip, core), own)]
        return remote(ref, ref, a1_s.at[d], a1_r.at[c, d], (to_right, to_left)[d])

    def a1_mate(g, d):
        c = lax.rem(g, CHUNKS)
        ref = hid.at[c, pl.ds(block_row(chip, core), own)]
        return remote(ref, ref, a1_s.at[d], a1_r.at[c, d], to_mate)

    def a2_copy(g, d):
        c = lax.rem(g, CHUNKS)
        base = pl.multiple_of(block_row((c_left, c_right)[d], core) + d * sub, sub)
        ref = hid.at[c, pl.ds(base, sub)]
        return remote(ref, ref, a2_s.at[d], a2_r.at[c, d], (to_right, to_left)[d])

    def d_copy(g, i, of=None):
        c = lax.rem(g, CHUNKS)
        ref = hid.at[c, pl.ds(block_row((chip, c_left, c_right, c_far)[i] if of is None else of, core), own)]
        return remote(ref, ref, d_s.at[i], d_r.at[c, i], to_pair)

    def by_stage(g, stage, then, other):
        is_it = lax.div(g, CHUNKS) == stage

        @pl.when(is_it)
        def _():
            then()

        @pl.when(jnp.logical_not(is_it))
        def _():
            other()

    def when_chunk(g, body):
        @pl.when(jnp.logical_and(g >= 0, g < n_steps))
        def _():
            body(g)

    def add_pair(g, gi):
        slot = lax.rem(g, 3)
        s = lax.rem(g, 2)

        @pl.loop(0, seg // PAD)
        def _(i):
            loc = pl.ds(pl.multiple_of(i * PAD, PAD), PAD)
            part[slot, gi, core, loc] = (part[slot, gi, core, loc].astype(F32) + pair_in[s, gi, loc].astype(F32)).astype(BF16)

    def e0(g):
        by_stage(g, swap_stage, lambda: half_pair_copy(g).start(), lambda: pair_copy(g).start())

    def e1(g):
        def swapped():
            half_pair_copy(g).wait_recv()
            half_pair_copy(g).wait_send()
            add_pair(g, grp)

        def usual():
            pair_copy(g).wait_recv()
            pair_copy(g).wait_send()
            for gi in range(2):
                add_pair(g, gi)
            for d in range(2):
                r1_copy(g, d).start()

        by_stage(g, swap_stage, swapped, usual)

    def e2(g):
        def usual():
            s = lax.rem(g, 2)
            for d in range(2):
                r1_copy(g, d).wait_send()
                r1_copy(g, d).wait_recv()
            for d in range(2):
                ref = part_block(g, (c_right, c_left)[d], d * sub, sub)
                ref[...] = (ref[...].astype(F32) + ring1[s, d].astype(F32)).astype(BF16)
                r2_copy(g, d).start()

        by_stage(g, swap_stage, lambda: r2_mate(g, mate_out).start(), usual)

    def e3(g):
        s = lax.rem(g, 2)
        c = lax.rem(g, CHUNKS)
        st = lax.div(g, CHUNKS)
        mine = part_block(g, chip, 0, own)
        base = block_row(chip, core)

        def finish(totals):
            def new_rows(i):
                loc = pl.ds(i * PAD, PAD)
                dst = pl.ds(pl.multiple_of(base + i * PAD, PAD), PAD)
                total = mine[loc].astype(F32)
                for d in totals:
                    total = total + ring2[s, d, loc].astype(F32)
                return loc, dst, (resid[c, loc].astype(F32) + total.astype(BF16).astype(F32)).astype(BF16)

            @pl.when(st < n_stage - 1)
            def _():
                gain = gains[jnp.minimum(st + 1, n_stage - 1)]
                for i in range(own // PAD):
                    loc, dst, new = new_rows(i)
                    resid[c, loc] = new
                    hid[c, dst] = norm_rows(new.astype(F32), gain)

            @pl.when(st == n_stage - 1)
            def _():
                for i in range(own // PAD):
                    _, dst, new = new_rows(i)
                    hid[c, dst] = new

        def swapped():
            r2_mate(g, mate_out).wait_send()
            r2_mate(g, mate_in).wait_recv()
            finish((mate_in,))

        def usual():
            for d in range(2):
                r2_copy(g, d).wait_send()
                r2_copy(g, d).wait_recv()
            finish((0, 1))

        by_stage(g, swap_stage, swapped, usual)

        def to_both():
            for d in range(2):
                a1_copy(g, d).start()

        by_stage(g, swap_stage - 1, lambda: a1_mate(g, mate_out).start(), to_both)
        d_copy(g, 0).start()

    def e4(g):
        def swapped():
            a1_mate(g, mate_out).wait_send()
            a1_mate(g, mate_in).wait_recv()
            d_copy(g, 0).wait_send()
            d_copy(g, 1, c_mate).start()

        def usual():
            for d in range(2):
                a1_copy(g, d).wait_send()
                a1_copy(g, d).wait_recv()
                a2_copy(g, d).start()
            d_copy(g, 0).wait_send()
            d_copy(g, 1).start()
            d_copy(g, 2).start()

        by_stage(g, swap_stage - 1, swapped, usual)

    def e5(g):
        def usual():
            for d in range(2):
                a2_copy(g, d).wait_send()
                a2_copy(g, d).wait_recv()
            d_copy(g, 1).wait_send()
            d_copy(g, 2).wait_send()
            d_copy(g, 3).start()

        by_stage(g, swap_stage - 1, lambda: d_copy(g, 1, c_mate).wait_send(), usual)

    def e6(g):
        def swapped():
            for i in range(2):
                d_copy(g, i).wait_recv()

        def usual():
            d_copy(g, 3).wait_send()
            for i in range(4):
                d_copy(g, i).wait_recv()

        by_stage(g, swap_stage - 1, swapped, usual)

    def y_pair_copy(st):
        return remote(y_part.at[st], y_pair.at[st], yp_s.at[st], yp_r.at[st], to_pair)

    def y_chip_copy(st, i):
        return remote(y_chip.at[st, chip], y_chip.at[st, chip], yc_s.at[i], yc_r.at[st, i], (to_right, to_left, to_far)[i])

    first_copy = remote(tail_out.at[:, pl.ds(0, d_model)], y_row, edge_s.at[0], edge_r.at[0], to_down)
    tail_copy = remote(tail_out, tail_in, edge_s.at[1], edge_r.at[1], to_up)

    def put_y(gain, at):
        row = norm_rows(y_row[...], gain)
        hid[CHUNKS - 1, pl.ds(at, PAD)] = jnp.broadcast_to(row.astype(F32), (PAD, d_model)).astype(BF16)

    def y_sum(st):
        y_pair_copy(st).wait_send()
        y_pair_copy(st).wait_recv()
        y_chip[st, chip] = y_part[st] + y_pair[st]
        for i in range(3):
            y_chip_copy(st, i).start()

    def y_done(st):
        for i in range(3):
            y_chip_copy(st, i).wait_send()
            y_chip_copy(st, i).wait_recv()
        total = y_chip[st, 0]
        for i in range(1, n_chip):
            total = total + y_chip[st, i]
        y_row[...] = y_row[...] + total.astype(BF16).astype(F32)

        @pl.when(st < n_stage - 1)
        def _():
            at = jnp.where(st + 1 == swap_stage, grp * half + half, rows)
            put_y(gains[jnp.minimum(st + 1, n_stage - 1)], pl.multiple_of(at, PAD))

        @pl.when(st == n_stage - 1)
        def _():
            tail_out[:, pl.ds(0, d_model)] = y_row[...]
            tail_copy.start()

    def c0_copy(layer):
        src = kv0 if layer == 0 else kv1.at[0]
        return remote(src, cb0.at[layer], c0_s.at[layer], c0_r.at[layer], to_up)

    def c1_copy(layer, i):
        def tokens(c):
            return pl.ds(pl.multiple_of(c * tok_chip, tok_chip), tok_chip)

        src, dst, to = (
            (cb0.at[layer, :, tokens(c_right)], cb1.at[layer, 0], to_right),
            (cb0.at[layer, :, tokens(c_left)], cb1.at[layer, 1], to_left),
            (cb0.at[layer, 0, tokens(c_far)], relay.at[layer, 0], to_right),
            (cb0.at[layer, 1, tokens(c_far)], relay.at[layer, 1], to_left),
            (relay.at[layer, 0], cb1.at[layer, 2, 0], to_right),
            (relay.at[layer, 1], cb1.at[layer, 2, 1], to_left),
        )[i]
        return remote(src, dst, c1_s.at[layer, i], c1_r.at[layer, i], to)

    def c2_source(layer, i, n, which):
        off = pl.multiple_of(which * tok_dev, tok_dev)
        if i < 3:
            return cb1.at[layer, i, n, pl.ds(off, tok_dev)], (c_left, c_right, c_far)[i]
        return cb0.at[layer, n, pl.ds(pl.multiple_of(chip * tok_chip + off, tok_dev), tok_dev)], chip

    def c2_copy(layer, i, n):
        src, src_chip = c2_source(layer, i, n, 1 - core)
        return remote(src, (k_tok, v_tok)[n].at[layer, 2 * src_chip + core], c2_s.at[layer, i, n], c2_r.at[layer, i, n], to_pair)

    def c2_local(layer, i, n):
        src, src_chip = c2_source(layer, i, n, core)
        return pltpu.make_async_copy(src, (k_tok, v_tok)[n].at[layer, 2 * src_chip + core], c2_l.at[layer, i, n])

    def cache_events(g):
        for layer in range(n_layers):
            at = CACHE_STEPS[layer]

            @pl.when(g == at[0])
            def _():
                c0_copy(layer).start()

            @pl.when(g == at[1])
            def _():
                c0_copy(layer).wait_send()
                c0_copy(layer).wait_recv()
                c1_copy(layer, 0).start()
                c1_copy(layer, 1).start()

            @pl.when(g == at[2])
            def _():
                c1_copy(layer, 2).start()
                c1_copy(layer, 3).start()

            @pl.when(g == at[3])
            def _():
                for i in (2, 3):
                    c1_copy(layer, i).wait_send()
                    c1_copy(layer, i).wait_recv()
                for i in (4, 5):
                    c1_copy(layer, i).start()

            @pl.when(g == at[4])
            def _():
                for i in (0, 1, 4, 5):
                    c1_copy(layer, i).wait_send()
                    c1_copy(layer, i).wait_recv()
                for i in range(4):
                    for n in range(2):
                        c2_copy(layer, i, n).start()
                        c2_local(layer, i, n).start()

            @pl.when(g == at[5])
            def _():
                for i in range(4):
                    for n in range(2):
                        c2_copy(layer, i, n).wait_send()
                        c2_copy(layer, i, n).wait_recv()
                        c2_local(layer, i, n).wait()

    n_wq = n_slots
    n_wx = len(WX_STEPS)
    o_piece = o_rows // n_ho // (n_wx - n_wq)

    def wx_ref(i, quarter, first=0, parts=1, given=False):
        size = (d_model // n_ho if i < n_wq else o_piece) // parts
        if i < n_wq:
            base = quarter * (d_model // n_ho)
            ref = w_qkv.at[swap_layer, i] if given else wq_x.at[i]
        else:
            base = quarter * (o_rows // n_ho) + (i - n_wq) * o_piece
            ref = w_o.at[swap_layer] if given else wo_x
        return ref.at[pl.ds(pl.multiple_of(base + first * size, size), size)]

    def wx_copy(i):
        return remote(wx_ref(i, ho, given=True), wx_ref(i, ho), wx_s.at[i], wx_r.at[i], to_swap)

    def wy_copy(i, j):
        ref = (
            wx_ref(i, ho),
            wx_ref(i, ho),
            wx_ref(i, lax.rem(ho + n_ho - 1, n_ho), 0, 2),
            wx_ref(i, lax.rem(ho + 1, n_ho), 1, 2),
        )[j]
        return remote(ref, ref, wy_s.at[i, j], wy_r.at[i, j], (to_up, to_down)[j % 2])

    def swap_events(g):
        for i in range(n_wx):
            @pl.when(g == WX_STEPS[i])
            def _():
                wx_copy(i).start()

    def share_events(g):
        for i in range(n_wx):
            share = WX_STEPS[i] + 2 + (i == n_wx - 2)

            @pl.when(g == share)
            def _():
                wx_copy(i).wait_send()
                wx_copy(i).wait_recv()
                for j in (0, 1):
                    wy_copy(i, j).start()

            @pl.when(g == share + 1)
            def _():
                for j in (0, 1):
                    wy_copy(i, j).wait_send()
                    wy_copy(i, j).wait_recv()
                for j in (2, 3):
                    wy_copy(i, j).start()

    def swap_arrived(pieces):
        for i in pieces:
            for j in (2, 3):
                wy_copy(i, j).wait_send()
                wy_copy(i, j).wait_recv()

    def store_part(g, t, acc):
        cols = pl.ds(pl.multiple_of(t * COLS_B, COLS_B), COLS_B)
        part[lax.rem(g, 3), :, :, :, cols] = acc[:rows].astype(BF16).reshape(2, 2, seg, COLS_B)
        y_part[lax.div(g, CHUNKS), :, cols] = acc[rows:rows + 1]

    def first_norm(c):
        prompt_copy(c).wait()
        gain = gains[0]
        for i in range(own // PAD):
            resid[c, pl.ds(i * PAD, PAD)] = hid[c, pl.ds(pl.multiple_of(block_row(chip, core) + i * PAD, PAD), PAD)]

        @pl.loop(0, rows // NORM_ROWS)
        def _(i):
            loc = pl.ds(pl.multiple_of(i * NORM_ROWS, NORM_ROWS), NORM_ROWS)
            hid[c, loc] = norm_rows(hid[c, loc].astype(F32), gain)

        @pl.when(c == CHUNKS - 1)
        def _():
            first_copy.wait_send()
            first_copy.wait_recv()
            put_y(gain, rows)

    def attention(c, keys, n_rows, row_of, before_diag, put):
        units = range(len(keys))

        def loc_of(j):
            return pl.ds(pl.multiple_of(j * rows, rows), rows)

        def score(u, loc):
            return lax.dot_general(qry[pl.ds(u * n_rows, n_rows)], keys[u][0, loc], CONTRACT_LAST, preferred_element_type=F32) * scale

        def fold(op, x, s):
            for b in range(rows // head):
                x = op(x, s[:, b * head:(b + 1) * head])
            return x

        def first(j, tops):
            loc = loc_of(j)
            new = []
            for u in units:
                s = score(u, loc)
                scores[pl.ds(u * n_rows, n_rows), loc] = s
                new.append(fold(jnp.maximum, tops[u], s))
            return tuple(new)

        lowest = jnp.full((n_rows, head), -jnp.inf, F32)
        tops = lax.fori_loop(0, c, first, tuple(lowest for _ in units))
        before_diag()
        diag = loc_of(c)
        causal = row_of(lax.broadcasted_iota(jnp.int32, (n_rows, rows), 0)) >= lax.broadcasted_iota(jnp.int32, (n_rows, rows), 1)
        row_top = []
        for u in units:
            s = jnp.where(causal, score(u, diag), -jnp.inf)
            scores[pl.ds(u * n_rows, n_rows), diag] = s
            row_top.append(jnp.max(fold(jnp.maximum, tops[u], s), axis=1, keepdims=True))

        def second(j, carry):
            loc = loc_of(j)
            new = []
            for u in units:
                denom, numer = carry[u]
                p = jnp.exp(scores[pl.ds(u * n_rows, n_rows), loc] - row_top[u])
                new.append((fold(jnp.add, denom, p), numer + jnp.dot(p.astype(BF16), keys[u][1, loc], preferred_element_type=F32)))
            return tuple(new)

        zero = jnp.zeros((n_rows, head), F32)
        sums = lax.fori_loop(0, c + 1, second, tuple((zero, zero) for _ in units))
        for u in units:
            denom, numer = sums[u]
            put(u, (numer / jnp.sum(denom, axis=1, keepdims=True)).astype(BF16))

    def attention_new(keys, att, at):
        q = qry_new[...].reshape(n_group * PAD, head)
        k_row = k_new[...].astype(F32)[:1]
        v_row = v_new[...].astype(F32)[:1]
        s_new = jnp.sum(q.astype(F32) * k_row, axis=1, keepdims=True) * scale
        s_old = lax.dot_general(q, keys[0], CONTRACT_LAST, preferred_element_type=F32) * scale
        top = jnp.maximum(jnp.max(s_old, axis=1, keepdims=True), s_new)
        p_old = jnp.exp(s_old - top)
        p_new = jnp.exp(s_new - top)
        denom = jnp.sum(p_old, axis=1, keepdims=True) + p_new
        numer = jnp.dot(p_old.astype(BF16), keys[1], preferred_element_type=F32) + p_new * v_row
        out = (numer / denom).astype(BF16)
        for h in range(n_group):
            att[pl.ds(at, PAD), pl.ds(h * head, head)] = out[h * PAD:(h + 1) * PAD]

    def put_new_kv(layer):
        tail_out[:, pl.ds(d_model + 2 * layer * head, head)] = k_new[...].astype(F32)[:1]
        tail_out[:, pl.ds(d_model + (2 * layer + 1) * head, head)] = v_new[...].astype(F32)[:1]

    def next_is_mlp(layer, c):
        @pl.when(c == CHUNKS - 1)
        def _():
            for t in range(2):
                start_gu(layer, t)

    def step_a(g, c):
        layer = 0
        first_norm(c)

        @pl.when(c == 0)
        def _():
            for t in range(t_qkv):
                for u in range(2):
                    qkv_copy(layer, t, u).wait()

        for t in range(t_qkv):
            out = jnp.dot(hid[c], wa[t], preferred_element_type=F32).astype(BF16)
            if t < t_qkv - 1:
                for u in range(2):
                    h = 2 * t + u
                    qry[pl.ds(h * rows, rows)] = out[:rows, u * head:(u + 1) * head]
                    qry_new[h] = out[rows:, u * head:(u + 1) * head]
            else:
                loc = pl.ds(pl.multiple_of(c * rows, rows), rows)
                kv0[0, loc] = out[:rows, :head]
                kv0[1, loc] = out[:rows, head:]
                k_new[...] = out[rows:, :head]
                v_new[...] = out[rows:, head:]

        next_is_mlp(layer, c)
        when_chunk(g - 1, e1)

        def put(u, o):
            att0[pl.ds(0, rows), pl.ds(u * head, head)] = o

        attention(c, [kv0] * n_group, rows, lambda r: r, lambda: None, put)

        @pl.when(c == CHUNKS - 1)
        def _():
            attention_new(kv0, att0, rows)
            put_new_kv(layer)

        @pl.when(c == 0)
        def _():
            for t in range(t_out):
                out_copy(layer, t).wait()

        for t in range(t_out):
            store_part(g, t, jnp.dot(att0[...], out_tile(t)[...], preferred_element_type=F32))

        @pl.when(c == CHUNKS - 1)
        def _():
            for t in range(SLOTS_B):
                down_copy(layer, 0, t).start()

    def kx_copy(c, o):
        loc = pl.ds(pl.multiple_of(c * rows + grp * half, half), half)
        return remote(kv1.at[o, :, loc], kv1.at[1 - o, :, loc], kx_s.at[o], kx_r.at[c, 1 - o], to_swap)

    def swap_qkv(c):
        lhs = pl.ds(pl.multiple_of(grp * half, half), half + PAD)
        loc = pl.ds(pl.multiple_of(c * rows + grp * half, half), half)
        for pair in range(t_qkv):
            slot = lax.rem(c * t_qkv + pair, 2) * 2
            for v in range(2):
                t = 2 * pair + v
                for u in range(2):
                    swap_qkv_copy(slot + v, t, u).wait()
                out = jnp.dot(hid[c, lhs], wa[slot + v], preferred_element_type=F32).astype(BF16)
                o, r = t // t_qkv, t % t_qkv
                if r < t_qkv - 1:
                    for u in range(2):
                        h = 2 * r + u
                        qry[pl.ds((o * n_group + h) * half, half)] = out[:half, u * head:(u + 1) * head]
                        if o == 0:
                            qry_new[h] = out[half:, u * head:(u + 1) * head]
                else:
                    kv1[o, 0, loc] = out[:half, :head]
                    kv1[o, 1, loc] = out[:half, head:]
                    if o == 0:
                        k_new[...] = out[half:, :head]
                        v_new[...] = out[half:, head:]

            if pair + 2 < t_qkv:
                start_swap_qkv(c, pair + 2)
            else:
                @pl.when(c + 1 < CHUNKS)
                def _():
                    start_swap_qkv(c + 1, pair + 2 - t_qkv)

        for o in range(2):
            kx_copy(c, o).start()

    def step_s(g, c):
        def before_diag():
            for o in range(2):
                kx_copy(c, o).wait_send()
                kx_copy(c, 1 - o).wait_recv()

        def put(u, out):
            for h in range(n_group):
                att1[pl.ds(0, half), pl.ds((u * n_group + h) * head, head)] = out[h * half:(h + 1) * half]

        attention(c, [kv1.at[0], kv1.at[1]], n_group * half, lambda r: lax.rem(r, half) + grp * half, before_diag, put)

        @pl.when(c == CHUNKS - 1)
        def _():
            attention_new(kv1.at[0], att1, half)
            put_new_kv(swap_layer)

        when_chunk(g - 1, e1)

    def swap_out(g, c):
        @pl.when(c == 0)
        def _():
            swap_arrived(range(n_wq, n_wx))
            for t in range(SLOTS_B):
                for v in range(2):
                    swap_out_copy(0, t, v).start()

        for t in range(t_out):
            slot = lax.rem(c * t_out + t, SLOTS_B)
            for v in range(2):
                swap_out_copy(c, t, v).wait()
            cols = pl.ds(t * COLS_B, COLS_B)
            acc = jnp.dot(att1[...], wb[slot, pl.ds(0, 2 * o_rows)], preferred_element_type=F32)
            part[lax.rem(g, 3), grp, :, :, cols] = acc[:half].astype(BF16).reshape(2, seg, COLS_B)
            y_part[swap_stage, :, cols] = acc[half:half + 1]
            ahead = t + SLOTS_B
            if ahead < t_out:
                for v in range(2):
                    swap_out_copy(c, ahead, v).start()
            else:
                @pl.when(c + 1 < CHUNKS)
                def _():
                    for v in range(2):
                        swap_out_copy(c + 1, ahead - t_out, v).start()

        @pl.when(c == CHUNKS - 1)
        def _():
            for t in range(SLOTS_B):
                down_copy(swap_layer, 0, t).start()

    def step_m(g, layer, c):
        more = layer < swap_layer

        @pl.loop(0, t_gu)
        def _(t):
            for u in range(2):
                gu_copy(layer, t, u).wait()
            slot = lax.rem(t, 2) * 2
            gate = jnp.dot(hid[c], wa[slot], preferred_element_type=F32)
            up = jnp.dot(hid[c], wa[slot + 1], preferred_element_type=F32)
            act[:, pl.ds(pl.multiple_of(t * COLS_A, COLS_A), COLS_A)] = (jax.nn.silu(gate) * up).astype(BF16)

            @pl.when(jnp.logical_or(t + 2 < t_gu, c + 1 < CHUNKS))
            def _():
                start_gu(layer, lax.rem(t + 2, t_gu))

        @pl.when(jnp.logical_and(c == CHUNKS - 1, more))
        def _():
            swap_arrived(range(n_wq))
            start_swap_qkv(0, 0)

        when_chunk(g - 1, e1)

        @pl.loop(0, t_out)
        def _(t):
            down_copy(layer, c, t).wait()
            store_part(g, t, jnp.dot(act[...], wb[lax.rem(c * t_out + t, SLOTS_B)], preferred_element_type=F32))
            ahead = t + SLOTS_B

            @pl.when(jnp.logical_or(ahead < t_out, c + 1 < CHUNKS))
            def _():
                down_copy(layer, c + lax.div(ahead, t_out), lax.rem(ahead, t_out)).start()

        @pl.when(jnp.logical_and(c == CHUNKS - 1, more))
        def _():
            start_swap_qkv(0, 1)

    for layer in range(n_layers):
        gains[2 * layer] = g_attn[layer:layer + 1]
        gains[2 * layer + 1] = g_mlp[layer:layer + 1]
    for c in range(CHUNKS):
        hid[c, pl.ds(rows, PAD)] = jnp.zeros((PAD, d_model), BF16)
    att0[pl.ds(rows, PAD)] = jnp.zeros((PAD, o_rows), BF16)
    att1[pl.ds(half, PAD)] = jnp.zeros((PAD, 2 * o_rows), BF16)
    pl.semaphore_wait(barrier, len(peers))
    first_copy.start()

    @pl.loop(0, n_steps + LAGS)
    def _(g):
        st = lax.div(g, CHUNKS)
        c = lax.rem(g, CHUNKS)
        layer = lax.div(st, 2)
        when_chunk(g - 6, e6)
        when_chunk(g - 5, e5)
        when_chunk(g - 4, e4)
        when_chunk(g - 3, e3)
        when_chunk(g - 2, e2)

        @pl.when(jnp.logical_and(c == 1, jnp.logical_and(st >= 1, st <= n_stage)))
        def _():
            y_sum(st - 1)

        @pl.when(jnp.logical_and(c == 2, jnp.logical_and(st >= 1, st <= n_stage)))
        def _():
            y_done(st - 1)

        share_events(g)

        @pl.when(g == 0)
        def _():
            swap_events(g)

        @pl.when(st == 0)
        def _():
            step_a(g, c)

        @pl.when(st == swap_stage)
        def _():
            step_s(g, c)

        @pl.when(jnp.logical_and(g < n_steps, lax.rem(st, 2) == 1))
        def _():
            step_m(g, layer, c)

        first_swap = swap_stage * CHUNKS - 1

        @pl.when(jnp.logical_and(g >= first_swap, g < first_swap + CHUNKS))
        def _():
            swap_qkv(g - first_swap)

        @pl.when(st == swap_stage)
        def _():
            swap_out(g, c)

        @pl.when(g == first_swap + CHUNKS - 1)
        def _():
            next_is_mlp(swap_layer, CHUNKS - 1)

        @pl.when(g > 0)
        def _():
            swap_events(g)

        cache_events(g)

        @pl.when(g == n_steps)
        def _():
            e1(g - 1)

        @pl.when(g < n_steps)
        def _():
            e0(g)

        @pl.when(jnp.logical_and(g < n_steps, c == CHUNKS - 1))
        def _():
            y_pair_copy(st).start()

    tail_copy.wait_send()
    tail_copy.wait_recv()
    tail[...] = tail_in[...]


def finish_kernel(hid, tail, k_tok, v_tok, x_last, k_cache, v_cache, y_last, kv_new, by_head, by_token, x_sem, in_sem, out_sem):
    n_layers = k_tok.shape[0]
    rows = x_last.shape[0] // CHUNKS
    d_model = y_last.shape[1]
    head = k_tok.shape[3]

    def x_copy(c):
        return pltpu.make_async_copy(hid.at[c, pl.ds(0, rows)], x_last.at[pl.ds(c * rows, rows)], x_sem.at[c])

    def in_copy(n):
        return pltpu.make_async_copy((k_tok, v_tok)[n], by_head.at[n], in_sem.at[n])

    def out_copy(n):
        return pltpu.make_async_copy(by_token.at[n], (k_cache, v_cache)[n], out_sem.at[n])

    for n in range(2):
        in_copy(n).start()
    for c in range(CHUNKS):
        x_copy(c).start()
    y_last[...] = tail[:, :d_model]
    kv_new[...] = jnp.concatenate([tail[:, d_model + i * head:d_model + (i + 1) * head] for i in range(2 * n_layers)], axis=0).astype(BF16)
    for n in range(2):
        in_copy(n).wait()
        for layer in range(n_layers):
            by_token[n, layer] = jnp.transpose(by_head[n, layer], (1, 0, 2))
        out_copy(n).start()
    for n in range(2):
        out_copy(n).wait()
    for c in range(CHUNKS):
        x_copy(c).wait()


def solution(mesh):
    n_ho, n_tp = mesh.shape['ho'], mesh.shape['tp']
    row_axes = ('pairs', 'ho')
    in_specs = (P('pairs'), P(row_axes), P(None, None, 'tp'), P(None, 'tp'), P(None, None, 'tp'), P(None, None, 'tp'), P(None, 'tp'), P(), P())
    out_specs = (P(row_axes), P(row_axes), P(row_axes, None, 'tp'), P(row_axes, None, 'tp'), P(row_axes, None, None, 'tp'))

    def device_program(prompts, y_first, w_qkv, w_o, w_gate, w_up, w_down, g_attn, g_mlp):
        n_layers, d_model, _, n_slots, head = w_qkv.shape
        n_tok = prompts.shape[1]
        ff = w_gate.shape[2]
        rows = n_tok // CHUNKS
        half = rows // 2
        seg = half // 2
        own = half // (n_tp // 2)
        n_stage = 2 * n_layers
        group = n_slots - 2
        o_rows = group * head
        tok_dev = n_tok // n_tp
        n_wx = len(WX_STEPS)
        wq = jnp.transpose(w_qkv[:, :, 0], (0, 2, 1, 3))
        tail_len = d_model + 2 * n_layers * head
        any_spec = pl.BlockSpec(memory_space=pl.ANY)
        vmem_spec = pl.BlockSpec(memory_space=pltpu.VMEM)
        hbm_spec = pl.BlockSpec(memory_space=pltpu.HBM)
        dma = pltpu.SemaphoreType.DMA
        both, both_ways, by_chunk, by_chunk_two = dma((2,)), dma((2, 2)), dma((CHUNKS,)), dma((CHUNKS, 2))
        by_stage, by_layer, cache = dma((n_stage,)), dma((n_layers,)), dma((n_layers, 4, 2))
        vmem = pltpu.VMEM
        hid, tail, k_tok, v_tok, *_ = pl.pallas_call(
            functools.partial(group_kernel, n_ho, n_tp),
            out_shape=(
                vmem((CHUNKS, rows + PAD, d_model), BF16),
                vmem((1, tail_len), F32),
                jax.ShapeDtypeStruct((n_layers, n_tp, tok_dev, head), BF16),
                jax.ShapeDtypeStruct((n_layers, n_tp, tok_dev, head), BF16),
                jax.ShapeDtypeStruct((n_slots, d_model, head), BF16),
                jax.ShapeDtypeStruct((o_rows, d_model), BF16),
                jax.ShapeDtypeStruct((n_layers, 2, n_tok, head), BF16),
                jax.ShapeDtypeStruct((n_layers, 3, 2, 2 * tok_dev, head), BF16),
                jax.ShapeDtypeStruct((n_layers, 2, 2 * tok_dev, head), BF16),
            ),
            in_specs=[any_spec, vmem_spec, any_spec, any_spec, any_spec, any_spec, any_spec, vmem_spec, vmem_spec],
            out_specs=(vmem_spec, vmem_spec) + (any_spec,) * 7,
            scratch_shapes=[
                vmem((3, 2, 2, seg, d_model), BF16),
                vmem((2, 2, seg, d_model), BF16),
                vmem((2, 2, own // 2, d_model), BF16),
                vmem((2, 2, own, d_model), BF16),
                vmem((CHUNKS, own, d_model), BF16),
                vmem((2, n_tok, head), BF16),
                vmem((2, 2, n_tok, head), BF16),
                vmem((group * rows, n_tok), F32),
                vmem((group * rows, head), BF16),
                vmem((group, PAD, head), BF16),
                vmem((rows + PAD, o_rows), BF16),
                vmem((half + PAD, 2 * o_rows), BF16),
                vmem((rows + PAD, ff), BF16),
                vmem((4, d_model, COLS_A), BF16),
                vmem((SLOTS_B, ff, COLS_B), BF16),
                vmem((PAD, head), BF16),
                vmem((PAD, head), BF16),
                vmem((n_stage, 1, d_model), F32),
                vmem((1, d_model), F32),
                vmem((n_stage, 1, d_model), F32),
                vmem((n_stage, 1, d_model), F32),
                vmem((n_stage, n_tp // 2, 1, d_model), F32),
                vmem((1, tail_len), F32),
                vmem((1, tail_len), F32),
                dma((4, 2)), dma((2 * SLOTS_B,)), by_chunk,
                both, both, both, both_ways, both, both_ways,
                both, by_chunk_two, both, by_chunk_two, dma((4,)), dma((CHUNKS, 4)),
                by_stage, by_stage, dma((3,)), dma((n_stage, 3)), both, both,
                by_layer, by_layer, dma((n_layers, 6)), dma((n_layers, 6)),
                cache, cache, cache,
                both, by_chunk_two, dma((n_wx,)), dma((n_wx,)), dma((n_wx, 4)), dma((n_wx, 4)),
            ],
            compiler_params=pltpu.CompilerParams(collective_id=0, has_side_effects=True, vmem_limit_bytes=VMEM_LIMIT),
            name="group_step",
        )(prompts, y_first, wq, w_o, w_gate, w_up, w_down, g_attn, g_mlp)
        x_last, k_cache, v_cache, y_last, kv_new = pl.pallas_call(
            finish_kernel,
            out_shape=(
                jax.ShapeDtypeStruct((n_tok, d_model), BF16),
                jax.ShapeDtypeStruct((n_layers, tok_dev, n_tp, head), BF16),
                jax.ShapeDtypeStruct((n_layers, tok_dev, n_tp, head), BF16),
                jax.ShapeDtypeStruct((1, d_model), F32),
                jax.ShapeDtypeStruct((2 * n_layers, head), BF16),
            ),
            in_specs=[any_spec, vmem_spec, hbm_spec, hbm_spec],
            out_specs=(any_spec, any_spec, any_spec, vmem_spec, vmem_spec),
            scratch_shapes=[
                vmem((2, n_layers, n_tp, tok_dev, head), BF16),
                vmem((2, n_layers, tok_dev, n_tp, head), BF16),
                by_chunk, both, both,
            ],
            compiler_params=pltpu.CompilerParams(vmem_limit_bytes=16 << 20),
            name="finish",
        )(hid, tail, *(pltpu.with_memory_space_constraint(tokens, pltpu.HBM) for tokens in (k_tok, v_tok)))
        kv_new = kv_new.reshape(n_layers, 2, 1, head)
        return x_last[None], y_last, k_cache[None], v_cache[None], kv_new[None]

    return jax.shard_map(device_program, mesh=mesh, in_specs=in_specs, out_specs=out_specs, check_vma=False)
```
